32 devices in a mesh: dp: 2 (over x), tp: 4 (over z), ep: 4 (over y, core).
Axes of the slice: x: 2, y: 2, z: 4, core: 2. Of those that a mesh axis runs over, the one named last changes fastest.
Arguments:
- hidden: bfloat16 [4096, 1536], P(('dp', 'ep')), parts along dimension 0
- expert_ids: int32 [4096, 8], P(('dp', 'ep')), parts along dimension 0
- norm_w: bfloat16 [1536], replicated
- router_w: bfloat16 [1536, 40], replicated
- w_gate: bfloat16 [40, 1536, 512], P('ep', None, 'tp')
- w_up: bfloat16 [40, 1536, 512], P('ep', None, 'tp')
- w_down: bfloat16 [40, 512, 1536], P('ep', 'tp')
Outputs:
- output: bfloat16 [4096, 1536], P(('dp', 'ep')), parts along dimension 0
There are 2 independent parts. The reference program is written for one: setup_inputs(seed, part) draws one part's arguments, and reference() takes and returns one part's arrays. A program takes and returns all parts, laid end to end along the dimension named above; an argument that names none is the same for every part.
All inputs are finite; a program needn't handle non-finite values.
Results may differ from the reference program's by a relative error of at most 0.0113036.
Values are sent between devices in bfloat16 or wider.
A program may use at most 1 GiB of HBM per device.

```python
import jax
import jax.numpy as jnp
from jax import lax

D = 1536
FF = 512
EXPERTS = 40
TOP = 8
TOK_DEV = 512
EP = 4
CAP = 208
TOKENS = TOK_DEV * EP
NORM_EPS = 1e-6


def random_order(order_key, count):
    order_score = jax.random.randint(order_key, (count,), 0, count) * count + jnp.arange(count, dtype=jnp.int32)
    return jnp.argsort(order_score)


def draw_routes(route_key):
    pair_count = TOP * TOK_DEV
    weight_total = (EXPERTS - 1) * (5 * EXPERTS - 2) // 2
    bounds = [CAP + ((pair_count - CAP) * (4 * rank_step * (EXPERTS - 1) - 3 * rank_step * (rank_step - 1) // 2)) // weight_total for rank_step in range(EXPERTS - 1)]
    bound_arr = jnp.array(bounds, dtype=jnp.int32)
    positions = jnp.arange(TOK_DEV, dtype=jnp.int32)[:, None] + TOK_DEV * jnp.arange(TOP, dtype=jnp.int32)[None, :]
    rank_of = jnp.sum((positions[:, :, None] >= bound_arr).astype(jnp.int32), axis=-1)
    label_key, rows_key = jax.random.split(route_key)
    labels = random_order(label_key, EXPERTS).astype(jnp.int32)
    choices = labels[rank_of]
    row_keys = jax.random.split(rows_key, EP)
    orders = jax.vmap(lambda sub_key: random_order(sub_key, TOK_DEV))(row_keys)
    return choices[orders].reshape(TOKENS, TOP).astype(jnp.int32)


def setup_inputs(seed: int = 0, part: int = 0) -> dict:
    base_key = jax.random.key(seed)
    key_list = jax.random.split(base_key, 7)
    hidden = jax.random.normal(jax.random.fold_in(key_list[0], part), (TOKENS, D), jnp.float32)
    expert_ids = draw_routes(jax.random.fold_in(key_list[1], part))
    norm_w = 1.0 + 0.3 * jax.random.normal(key_list[2], (D,), jnp.float32)
    router_w = D ** -0.5 * jax.random.normal(key_list[3], (D, EXPERTS), jnp.float32)
    w_gate = D ** -0.5 * jax.random.normal(key_list[4], (EXPERTS, D, FF), jnp.float32)
    w_up = D ** -0.5 * jax.random.normal(key_list[5], (EXPERTS, D, FF), jnp.float32)
    down_scale = 2.0 * EXPERTS / (TOP * FF) ** 0.5
    w_down = down_scale * jax.random.normal(key_list[6], (EXPERTS, FF, D), jnp.float32)
    return {"hidden": hidden.astype(jnp.bfloat16), "expert_ids": expert_ids, "norm_w": norm_w.astype(jnp.bfloat16), "router_w": router_w.astype(jnp.bfloat16), "w_gate": w_gate.astype(jnp.bfloat16), "w_up": w_up.astype(jnp.bfloat16), "w_down": w_down.astype(jnp.bfloat16)}


def rms_norm(hidden, norm_w):
    wide_h = hidden.astype(jnp.float32)
    mean_sq = jnp.mean(wide_h * wide_h, axis=-1, keepdims=True)
    return (wide_h * lax.rsqrt(mean_sq + NORM_EPS) * norm_w.astype(jnp.float32)).astype(jnp.bfloat16)


def reference(hidden, expert_ids, norm_w, router_w, w_gate, w_up, w_down):
    normed = rms_norm(hidden, norm_w)
    logits = jnp.dot(normed, router_w, preferred_element_type=jnp.float32)
    router_prob = jax.nn.softmax(logits, axis=-1)
    gate_prob = jnp.take_along_axis(router_prob, expert_ids, axis=-1).reshape(-1)
    flat_ids = expert_ids.reshape(-1)
    pair_tok = jnp.arange(TOKENS * TOP, dtype=jnp.int32) // TOP
    row_limit = EP * CAP

    def one_expert(accum, per_expert):
        expert, gate_e, up_e, down_e = per_expert
        chosen = flat_ids == expert
        (picked,) = jnp.nonzero(chosen, size=row_limit, fill_value=0)
        row_valid = jnp.arange(row_limit) < jnp.sum(chosen.astype(jnp.int32))
        tok_rows = pair_tok[picked]
        x_rows = normed[tok_rows]
        gate_pre = jnp.dot(x_rows, gate_e, preferred_element_type=jnp.float32)
        up_pre = jnp.dot(x_rows, up_e, preferred_element_type=jnp.float32)
        act_rows = (jax.nn.silu(gate_pre) * up_pre).astype(jnp.bfloat16)
        expert_out = jnp.dot(act_rows, down_e, preferred_element_type=jnp.float32).astype(jnp.bfloat16)
        weight = jnp.where(row_valid, gate_prob[picked], 0.0)
        return accum.at[tok_rows].add(weight[:, None] * expert_out.astype(jnp.float32)), None

    moe_sum, _ = lax.scan(one_expert, jnp.zeros((TOKENS, D), jnp.float32), (jnp.arange(EXPERTS, dtype=jnp.int32), w_gate, w_up, w_down))
    return (hidden.astype(jnp.float32) + moe_sum).astype(jnp.bfloat16)
```

```python
import jax
import jax.numpy as jnp
from jax import lax
from jax.sharding import PartitionSpec as P

NORM_EPS = 1e-6


def rms_norm(hidden, norm_w):
    wide_h = hidden.astype(jnp.float32)
    mean_sq = jnp.mean(wide_h * wide_h, axis=-1, keepdims=True)
    return (wide_h * lax.rsqrt(mean_sq + NORM_EPS) * norm_w.astype(jnp.float32)).astype(jnp.bfloat16)


def solution(mesh):
    def per_device(hidden, expert_ids, norm_w, router_w, w_gate, w_up, w_down):
        tok_dev, model_dim = hidden.shape
        n_experts = router_w.shape[1]
        local_exp, _, width = w_gate.shape
        normed = rms_norm(hidden, norm_w)
        logits = jnp.dot(normed, router_w, preferred_element_type=jnp.float32)
        prob = jax.nn.softmax(logits, axis=-1)
        chosen = jnp.any(expert_ids[:, :, None] == jnp.arange(n_experts, dtype=jnp.int32)[None, None, :], axis=1)
        gates = jnp.where(chosen, prob, 0.0)
        all_rows = lax.all_gather(normed, "ep", axis=0, tiled=True)
        all_gates = lax.all_gather(gates, "ep", axis=0, tiled=True)
        my_gates = lax.dynamic_slice_in_dim(all_gates, lax.axis_index("ep") * local_exp, local_exp, axis=1)
        gate_pre = jnp.einsum("td,edf->etf", all_rows, w_gate, preferred_element_type=jnp.float32)
        up_pre = jnp.einsum("td,edf->etf", all_rows, w_up, preferred_element_type=jnp.float32)
        act = (jax.nn.silu(gate_pre) * up_pre).astype(jnp.bfloat16).astype(jnp.float32)
        act = (act * my_gates.T[:, :, None]).astype(jnp.bfloat16)
        part = jnp.einsum("etf,efd->td", act, w_down, preferred_element_type=jnp.float32).astype(jnp.bfloat16)
        mine = lax.psum_scatter(part, "ep", scatter_dimension=0, tiled=True)
        total = lax.psum(mine, "tp")
        return (hidden.astype(jnp.float32) + total.astype(jnp.float32)).astype(jnp.bfloat16)

    token_spec = P(("dp", "ep"), None)
    return jax.shard_map(per_device, mesh=mesh, in_specs=(token_spec, token_spec, P(None), P(None, None), P("ep", None, "tp"), P("ep", None, "tp"), P("ep", "tp", None)), out_specs=token_spec, check_vma=False)
```

```python
import functools

import jax
import jax.numpy as jnp
from jax import lax
from jax.experimental import pallas as pl
from jax.experimental.pallas import tpu as pltpu
from jax.sharding import PartitionSpec as P

NORM_EPS = 1e-6
MESH = pl.DeviceIdType.MESH
OWN_SLOT = (0, 1, 2, 5)
FAR_SLOT = (3, 4, 6, 7)
N_SUB = 4
PIECE = 32


def body(n_experts, ids_ref, h_ref, nw_ref, wr_ref, wg_hbm, wu_hbm, wd_hbm, out_hbm,
         v, wgu, wd, act, keep, dsend, drecv, sbuf, rbuf, tbuf, abuf, ubuf, obuf, ids_all, ids_slot,
         w_sem, ids_s, ids_r, d1_s, d1_r, dy_s, dy_r, dz_s, dz_r, dd_s, dd_r, pd_s, pd_r,
         sy_s, sy_r, ra_s, ra_r, rb_s, rb_r, rc_s, rc_r, o_sem):
    tok, dim = h_ref.shape
    local_exp, _, width = wg_hbm.shape
    sub = tok // N_SUB
    half = sub // 2
    n_piece = tok // PIECE
    per_sub = sub // PIECE
    ep = lax.axis_index("ep")
    z = lax.axis_index("tp")
    core, y = ep % 2, ep // 2
    ep_pair = 2 * y + 1 - core
    ep_far = 2 * (1 - y) + core
    ep_diag = 2 * (1 - y) + 1 - core
    side = z % 2
    z_pair = z + 1 - 2 * side
    z_mirror = 3 - z
    inner = jnp.logical_or(z == 1, z == 2)
    outer = jnp.logical_or(z == 0, z == 3)

    def remote(src, dst, ssem, rsem, **where):
        return pltpu.make_async_remote_copy(src_ref=src, dst_ref=dst, send_sem=ssem, recv_sem=rsem, device_id=where, device_id_type=MESH)

    def weight_copies():
        copies = []
        for e in range(local_exp):
            copies.append(pltpu.make_async_copy(wg_hbm.at[e], wgu.at[e, :, pl.ds(0, width)], w_sem.at[2 * e]))
            copies.append(pltpu.make_async_copy(wu_hbm.at[e], wgu.at[e, :, pl.ds(width, width)], w_sem.at[2 * e + 1]))
        copies.append(pltpu.make_async_copy(wd_hbm, wd, w_sem.at[2 * local_exp]))
        return copies

    barrier = pltpu.get_barrier_semaphore()
    for where in ({"ep": ep_pair}, {"ep": ep_far}, {"ep": ep_diag}, {"tp": z_pair}, {"tp": z_mirror}):
        pl.semaphore_signal(barrier, inc=1, device_id=where, device_id_type=MESH)
    for copy in weight_copies():
        copy.start()

    def norm_rows(s):
        slot = OWN_SLOT[s]

        def group(i, carry):
            r = pl.multiple_of(i * 16, 16)
            x = h_ref[pl.ds(s * sub + r, 16), :].astype(jnp.float32)
            ms = jnp.mean(x * x, axis=-1, keepdims=True)
            v[slot, pl.ds(r, 16), :] = (x * lax.rsqrt(ms + NORM_EPS) * nw_ref[...].astype(jnp.float32)).astype(jnp.bfloat16)
            return carry

        lax.fori_loop(0, sub // 16, group, 0)

    def half_rows(which):
        return pl.ds(pl.multiple_of(which * half, half), half)

    def ids_copy(k):
        ep_to = (ep_pair, ep_far, ep_diag)[k]
        return remote(ids_ref, ids_all.at[k], ids_s.at[k], ids_r.at[k], ep=ep_to)

    def d1(s):
        slot = OWN_SLOT[s]
        return remote(v.at[slot, pl.ds(0, sub)], v.at[slot, pl.ds(sub, sub)], d1_s.at[s], d1_r.at[s], ep=ep_pair)

    def dy(s):
        rows = half_rows(side)
        return remote(v.at[OWN_SLOT[s], rows], v.at[FAR_SLOT[s], rows], dy_s.at[s], dy_r.at[s], ep=ep_far)

    def dz(s):
        rows = half_rows(side)
        return remote(v.at[FAR_SLOT[s], rows], v.at[FAR_SLOT[s], rows], dz_s.at[s], dz_r.at[s], tp=z_pair)

    def dz_in(s):
        rows = half_rows(1 - side)
        return remote(v.at[FAR_SLOT[s], rows], v.at[FAR_SLOT[s], rows], dz_s.at[s], dz_r.at[s], tp=z_pair)

    def dd(s, k):
        which = side if k == 0 else 1 - side
        src = pl.ds(pl.multiple_of(which * half, half), half)
        dst = pl.ds(pl.multiple_of(sub + which * half, half), half)
        return remote(v.at[FAR_SLOT[s], src], v.at[FAR_SLOT[s], dst], dd_s.at[2 * s + k], dd_r.at[2 * s + k], ep=ep_pair)

    def pd(slot):
        return remote(dsend.at[slot], drecv.at[slot], pd_s.at[slot], pd_r.at[slot], ep=ep_pair)

    def piece_rows(p):
        return pl.ds(pl.multiple_of(p * PIECE, PIECE), PIECE)

    def sy(p):
        return remote(sbuf.at[piece_rows(p)], rbuf.at[piece_rows(p)], sy_s.at[p], sy_r.at[p], ep=ep_far)

    def ra(p):
        return remote(tbuf.at[piece_rows(p)], abuf.at[piece_rows(p)], ra_s.at[p], ra_r.at[p], tp=z_pair)

    def rb(p):
        return remote(tbuf.at[piece_rows(p)], ubuf.at[piece_rows(p)], rb_s.at[p], rb_r.at[p], tp=z_mirror)

    def rc(p):
        return remote(obuf.at[piece_rows(p)], obuf.at[piece_rows(p)], rc_s.at[p], rc_r.at[p], tp=z_pair)

    def out_copy(p):
        return pltpu.make_async_copy(obuf.at[piece_rows(p)], out_hbm.at[piece_rows(p)], o_sem.at[p])

    norm_rows(0)
    pl.semaphore_wait(barrier, 5)
    for s in range(N_SUB):
        if s:
            norm_rows(s)
        dy(s).start()
        d1(s).start()
        if s == 0:
            for k in range(3):
                ids_copy(k).start()

    def far_in(s):
        dy(s).wait_recv()
        dz(s).start()
        dd(s, 0).start()

    def far_pair_in(s):
        dz_in(s).wait_recv()
        dd(s, 1).start()

    def far_ready(s):
        dd(s, 0).wait_recv()
        dd(s, 1).wait_recv()

    def ids_own():
        ids_copy(0).wait_recv()
        for s in range(N_SUB):
            ids_slot[OWN_SLOT[s], 0] = ids_ref[s]
            ids_slot[OWN_SLOT[s], 1] = ids_all[0, s]

    def ids_far():
        ids_copy(1).wait_recv()
        ids_copy(2).wait_recv()
        for s in range(N_SUB):
            ids_slot[FAR_SLOT[s], 0] = ids_all[1, s]
            ids_slot[FAR_SLOT[s], 1] = ids_all[2, s]

    def far_sum(s):
        slot = FAR_SLOT[s]
        pd(slot).wait_recv()

        def one(i, carry):
            r = pl.multiple_of(i * PIECE, PIECE)
            total = keep[slot, pl.ds(r, PIECE), :] + drecv[slot, pl.ds(r, PIECE), :].astype(jnp.float32)
            sbuf[pl.ds(s * sub + r, PIECE), :] = total.astype(jnp.bfloat16)
            sy(s * per_sub + i).start()
            return carry

        lax.fori_loop(0, per_sub, one, 0)

    for copy in weight_copies():
        copy.wait()

    pre = {0: [lambda: d1(0).wait_recv(), ids_own],
           1: [lambda: d1(1).wait_recv()],
           2: [lambda: d1(2).wait_recv()],
           3: [lambda: far_pair_in(0), ids_far, lambda: far_ready(0)],
           4: [lambda: far_ready(1)],
           5: [lambda: d1(3).wait_recv()],
           6: [lambda: far_pair_in(3), lambda: far_ready(2)],
           7: [lambda: far_ready(3)]}
    mid = {1: [lambda: far_in(0)],
           2: [lambda: far_in(1)],
           3: [lambda: far_in(2), lambda: far_pair_in(1)],
           4: [lambda: far_in(3), lambda: far_sum(0)],
           5: [lambda: far_pair_in(2), lambda: far_sum(1)],
           7: [lambda: far_sum(2)]}

    def run(tasks, step):
        for k, fns in tasks.items():
            @pl.when(step == k)
            def _(fns=fns):
                for fn in fns:
                    fn()

    def chosen_of(tile):
        expert = lax.broadcasted_iota(jnp.int32, (16, sub), 0) + ep * local_exp
        hit = jnp.zeros((16, sub), jnp.float32)
        for j in range(tile.shape[0]):
            hit = jnp.where(tile[j:j + 1, :] == expert, 1.0, hit)
        full = jnp.concatenate([hit, jnp.zeros((sub - 16, sub), jnp.float32)], axis=0)
        return full.T

    @pl.loop(0, 2 * N_SUB)
    def _(step):
        run(pre, step)
        x = v.at[step]
        logits = jnp.dot(x[...], wr_ref[...], preferred_element_type=jnp.float32)
        lane = lax.broadcasted_iota(jnp.int32, logits.shape, 1)
        logits = jnp.where(lane < n_experts, logits, -jnp.inf)
        raised = jnp.exp(logits - jnp.max(logits, axis=-1, keepdims=True))
        prob = raised / jnp.sum(raised, axis=-1, keepdims=True)
        chosen = jnp.concatenate([chosen_of(ids_slot[step, 0]), chosen_of(ids_slot[step, 1])], axis=0)
        gates = prob * chosen
        for e in range(local_exp):
            gu = jnp.dot(x[...], wgu[e], preferred_element_type=jnp.float32)
            a = (jax.nn.silu(gu[:, :width]) * gu[:, width:]).astype(jnp.bfloat16).astype(jnp.float32)
            act[:, e * width:(e + 1) * width] = (a * gates[:, e:e + 1]).astype(jnp.bfloat16)
        run(mid, step)
        cols = 512
        for n in range(dim // cols):
            part = jnp.dot(act[...], wd[:, n * cols:(n + 1) * cols], preferred_element_type=jnp.float32)
            keep[step, :, n * cols:(n + 1) * cols] = part[:sub]
            dsend[step, :, n * cols:(n + 1) * cols] = part[sub:].astype(jnp.bfloat16)
        pd(step).start()

    far_sum(3)
    for s in range(N_SUB):
        pd(OWN_SLOT[s]).wait_recv()

    def stage_b(p):
        rb(p).wait_recv()
        rows = piece_rows(p)
        total = tbuf[rows, :].astype(jnp.float32) + ubuf[rows, :].astype(jnp.float32)
        obuf[rows, :] = (h_ref[rows, :].astype(jnp.float32) + total).astype(jnp.bfloat16)
        rc(p).start()
        out_copy(p).start()

    @pl.loop(0, n_piece)
    def _(p):
        s = p // per_sub
        slot = s + 2 * (s // 3)
        rows = piece_rows(p)
        in_slot = pl.ds(pl.multiple_of((p - s * per_sub) * PIECE, PIECE), PIECE)
        sy(p).wait_recv()
        total = keep[slot, in_slot, :] + drecv[slot, in_slot, :].astype(jnp.float32) + rbuf[rows, :].astype(jnp.float32)

        @pl.when(outer)
        def _():
            tbuf[rows, :] = total.astype(jnp.bfloat16)
            ra(p).start()

        @pl.when(inner)
        def _():
            ra(p).wait_recv()
            tbuf[rows, :] = (total + abuf[rows, :].astype(jnp.float32)).astype(jnp.bfloat16)
            rb(p).start()

            @pl.when(p > 0)
            def _():
                stage_b(p - 1)

    @pl.when(inner)
    def _():
        stage_b(n_piece - 1)

    @pl.when(outer)
    def _():
        @pl.loop(0, n_piece)
        def _(p):
            rc(p).wait_recv()
            out_copy(p).start()

    for k in range(3):
        ids_copy(k).wait_send()
    for s in range(N_SUB):
        d1(s).wait_send()
        dy(s).wait_send()
        dz(s).wait_send()
        dd(s, 0).wait_send()
        dd(s, 1).wait_send()

    @pl.loop(0, 2 * N_SUB)
    def _(slot):
        pd(slot).wait_send()

    @pl.loop(0, n_piece)
    def _(p):
        sy(p).wait_send()
        out_copy(p).wait()

        @pl.when(outer)
        def _():
            ra(p).wait_send()

        @pl.when(inner)
        def _():
            rb(p).wait_send()
            rc(p).wait_send()


def solution(mesh):
    def per_device(hidden, expert_ids, norm_w, router_w, w_gate, w_up, w_down):
        tok, dim = hidden.shape
        top_k = expert_ids.shape[1]
        n_experts = router_w.shape[1]
        local_exp, _, width = w_gate.shape
        sub = tok // N_SUB
        n_piece = tok // PIECE
        my_first = lax.axis_index("ep") * local_exp
        doubled = jnp.concatenate([router_w, router_w], axis=1)
        turned = lax.dynamic_slice_in_dim(doubled, my_first, n_experts, axis=1)
        turned = jnp.pad(turned, ((0, 0), (0, 128 - n_experts)))
        ids_t = expert_ids.reshape(N_SUB, sub, top_k).transpose(0, 2, 1)
        bf, f32 = jnp.bfloat16, jnp.float32
        vmem = pl.BlockSpec(memory_space=pltpu.VMEM)
        hbm = pl.BlockSpec(memory_space=pl.ANY)
        dma = pltpu.SemaphoreType.DMA
        scratch = [
            pltpu.VMEM((2 * N_SUB, 2 * sub, dim), bf),
            pltpu.VMEM((local_exp, dim, 2 * width), bf),
            pltpu.VMEM((local_exp * width, dim), bf),
            pltpu.VMEM((2 * sub, local_exp * width), bf),
            pltpu.VMEM((2 * N_SUB, sub, dim), f32),
            pltpu.VMEM((2 * N_SUB, sub, dim), bf),
            pltpu.VMEM((2 * N_SUB, sub, dim), bf),
            pltpu.VMEM((tok, dim), bf),
            pltpu.VMEM((tok, dim), bf),
            pltpu.VMEM((tok, dim), bf),
            pltpu.VMEM((tok, dim), bf),
            pltpu.VMEM((tok, dim), bf),
            pltpu.VMEM((tok, dim), bf),
            pltpu.VMEM((3, N_SUB, top_k, sub), jnp.int32),
            pltpu.VMEM((2 * N_SUB, 2, top_k, sub), jnp.int32),
            dma((2 * local_exp + 1,)),
            dma((3,)), dma((3,)),
            dma((N_SUB,)), dma((N_SUB,)),
            dma((N_SUB,)), dma((N_SUB,)),
            dma((N_SUB,)), dma((N_SUB,)),
            dma((2 * N_SUB,)), dma((2 * N_SUB,)),
            dma((2 * N_SUB,)), dma((2 * N_SUB,)),
            dma((n_piece,)), dma((n_piece,)),
            dma((n_piece,)), dma((n_piece,)),
            dma((n_piece,)), dma((n_piece,)),
            dma((n_piece,)), dma((n_piece,)),
            dma((n_piece,)),
        ]
        return pl.pallas_call(
            functools.partial(body, n_experts),
            out_shape=jax.ShapeDtypeStruct((tok, dim), bf),
            in_specs=[vmem, vmem, vmem, vmem, hbm, hbm, hbm],
            out_specs=hbm,
            scratch_shapes=scratch,
            compiler_params=pltpu.CompilerParams(collective_id=0, has_side_effects=True, vmem_limit_bytes=64_000_000),
            name="moe_layer",
        )(ids_t, hidden, norm_w.reshape(1, dim), turned, w_gate, w_up, w_down.reshape(local_exp * width, dim))

    token_spec = P(("dp", "ep"), None)
    return jax.shard_map(per_device, mesh=mesh, in_specs=(token_spec, token_spec, P(None), P(None, None), P("ep", None, "tp"), P("ep", None, "tp"), P("ep", "tp", None)), out_specs=token_spec, check_vma=False)
```

```python
import jax
import jax.numpy as jnp
from jax import lax
from jax.experimental import pallas as pl
from jax.experimental.pallas import tpu as pltpu
from jax.sharding import PartitionSpec as P

NORM_EPS = 1e-6
MESH = pl.DeviceIdType.MESH
OWN_SLOT = (0, 1, 2, 4)
FAR_SLOT = (3, 5, 6, 7)
N_SUB = 4
UNITS = ((0, 0, 32), (0, 32, 32), (1, 0, 64), (2, 0, 64), (3, 0, 64))
COLS = 512
PIECE = 16


def body(ids_hbm, h_hbm, nw_hbm, wrt_hbm, wg_hbm, wu_hbm, wd_hbm, out_ref,
         ids_ref, nw_ref, wrt_ref, h_ref, wr, v, wgu, wd, act, keep, dsend, drecv, sbuf, rbuf, tbuf, abuf, ubuf, ids_all, ids_slot,
         h_sem, w_sem, ids_s, ids_r, d1_s, d1_r, dy_s, dy_r, dz_s, dz_r, dd_s, dd_r, pd_s, pd_r,
         sy_s, sy_r, ra_s, ra_r, rb_s, rb_r, rc_s, rc_r):
    tok, dim = h_ref.shape
    n_experts = wrt_ref.shape[0]
    local_exp, _, width = wg_hbm.shape
    sub = tok // N_SUB
    half = sub // 2
    n_piece = tok // PIECE
    per_sub = sub // PIECE
    ep = lax.axis_index("ep")
    z = lax.axis_index("tp")
    core, y = ep % 2, ep // 2
    ep_pair = 2 * y + 1 - core
    ep_far = 2 * (1 - y) + core
    ep_diag = 2 * (1 - y) + 1 - core
    side = z % 2
    z_pair = z + 1 - 2 * side
    z_mirror = 3 - z
    inner = jnp.logical_or(z == 1, z == 2)
    outer = jnp.logical_or(z == 0, z == 3)

    def remote(src, dst, ssem, rsem, **where):
        return pltpu.make_async_remote_copy(src_ref=src, dst_ref=dst, send_sem=ssem, recv_sem=rsem, device_id=where, device_id_type=MESH)

    def weight_copies():
        copies = []
        for e in range(local_exp):
            copies.append(pltpu.make_async_copy(wg_hbm.at[e], wgu.at[e, :, pl.ds(0, width)], w_sem.at[2 * e]))
            copies.append(pltpu.make_async_copy(wu_hbm.at[e], wgu.at[e, :, pl.ds(width, width)], w_sem.at[2 * e + 1]))
        copies.append(pltpu.make_async_copy(wd_hbm, wd, w_sem.at[2 * local_exp]))
        return copies

    def h_copy(s):
        rows = pl.ds(s * sub, sub)
        return pltpu.make_async_copy(h_hbm.at[rows], h_ref.at[rows], h_sem.at[s])

    small = [pltpu.make_async_copy(src, dst, h_sem.at[N_SUB + k]) for k, (src, dst) in enumerate(((nw_hbm, nw_ref), (ids_hbm, ids_ref), (wrt_hbm, wrt_ref)))]
    h_copy(0).start()
    for copy in small:
        copy.start()
    for s in range(1, N_SUB):
        h_copy(s).start()
    barrier = pltpu.get_barrier_semaphore()
    for where in ({"ep": ep_pair}, {"ep": ep_far}, {"ep": ep_diag}, {"tp": z_pair}, {"tp": z_mirror}):
        pl.semaphore_signal(barrier, inc=1, device_id=where, device_id_type=MESH)
    weights = weight_copies()
    for copy in weights:
        copy.start()

    small[0].wait()
    scale = nw_ref[...].astype(jnp.float32).reshape(1, dim)

    def norm_rows(s):
        slot = OWN_SLOT[s]

        h_copy(s).wait()

        def group(i, carry):
            r = pl.multiple_of(i * 16, 16)
            x = h_ref[pl.ds(s * sub + r, 16), :].astype(jnp.float32)
            ms = jnp.mean(x * x, axis=-1, keepdims=True)
            v[slot, pl.ds(r, 16), :] = (x * lax.rsqrt(ms + NORM_EPS) * scale).astype(jnp.bfloat16)
            return carry

        lax.fori_loop(0, sub // 16, group, 0, unroll=4)

    def unit_rows(u, which, base=0):
        _, first, rows = UNITS[u]
        return pl.ds(pl.multiple_of(base + which * half + first, 16), rows)

    def ids_copy(k):
        ep_to = (ep_pair, ep_far, ep_diag)[k]
        return remote(ids_ref, ids_all.at[k], ids_s.at[k], ids_r.at[k], ep=ep_to)

    def d1(s):
        slot = OWN_SLOT[s]
        return remote(v.at[slot, pl.ds(0, sub)], v.at[slot, pl.ds(sub, sub)], d1_s.at[s], d1_r.at[s], ep=ep_pair)

    def dy(u):
        s, rows = UNITS[u][0], unit_rows(u, side)
        return remote(v.at[OWN_SLOT[s], rows], v.at[FAR_SLOT[s], rows], dy_s.at[u], dy_r.at[u], ep=ep_far)

    def dz(u, which):
        s, rows = UNITS[u][0], unit_rows(u, which)
        return remote(v.at[FAR_SLOT[s], rows], v.at[FAR_SLOT[s], rows], dz_s.at[u], dz_r.at[u], tp=z_pair)

    def dd(u, k):
        s, which = UNITS[u][0], side if k == 0 else 1 - side
        return remote(v.at[FAR_SLOT[s], unit_rows(u, which)], v.at[FAR_SLOT[s], unit_rows(u, which, sub)], dd_s.at[2 * u + k], dd_r.at[2 * u + k], ep=ep_pair)

    def pd(slot, n):
        cols = pl.ds(n * COLS, COLS)
        k = slot * (dim // COLS) + n
        return remote(dsend.at[slot, :, cols], drecv.at[slot, :, cols], pd_s.at[k], pd_r.at[k], ep=ep_pair)

    def pair_part(slot):
        for n in range(dim // COLS):
            pd(slot, n).wait_recv()

    def piece_rows(p):
        return pl.ds(pl.multiple_of(p * PIECE, PIECE), PIECE)

    def sy(p):
        return remote(sbuf.at[piece_rows(p)], rbuf.at[piece_rows(p)], sy_s.at[p], sy_r.at[p], ep=ep_far)

    def ra(p):
        return remote(tbuf.at[piece_rows(p)], abuf.at[piece_rows(p)], ra_s.at[p], ra_r.at[p], tp=z_pair)

    def rb(p):
        return remote(tbuf.at[piece_rows(p)], ubuf.at[piece_rows(p)], rb_s.at[p], rb_r.at[p], tp=z_mirror)

    def rc(p):
        return remote(out_ref.at[piece_rows(p)], out_ref.at[piece_rows(p)], rc_s.at[p], rc_r.at[p], tp=z_pair)

    norm_rows(0)
    pl.semaphore_wait(barrier, 5)
    for s in range(N_SUB):
        if s:
            norm_rows(s)
        for u, unit in enumerate(UNITS):
            if unit[0] == s:
                dy(u).start()
        d1(s).start()
        if s == 0:
            small[1].wait()
            for k in range(3):
                ids_copy(k).start()

    def far_in(u):
        dy(u).wait_recv()
        dz(u, side).start()
        dd(u, 0).start()

    def far_pair_in(u):
        dz(u, 1 - side).wait_recv()
        dd(u, 1).start()

    def far_ready(s):
        for u, unit in enumerate(UNITS):
            if unit[0] == s:
                dd(u, 0).wait_recv()
                dd(u, 1).wait_recv()

    def ids_own():
        ids_copy(0).wait_recv()
        for s in range(N_SUB):
            ids_slot[OWN_SLOT[s], 0] = ids_ref[s]
            ids_slot[OWN_SLOT[s], 1] = ids_all[0, s]

    def ids_far():
        ids_copy(1).wait_recv()
        ids_copy(2).wait_recv()
        for s in range(N_SUB):
            ids_slot[FAR_SLOT[s], 0] = ids_all[1, s]
            ids_slot[FAR_SLOT[s], 1] = ids_all[2, s]

    def far_sum(s):
        slot = FAR_SLOT[s]
        pair_part(slot)

        def one(i, carry):
            r = pl.multiple_of(i * PIECE, PIECE)
            total = keep[slot, pl.ds(r, PIECE), :] + drecv[slot, pl.ds(r, PIECE), :].astype(jnp.float32)
            sbuf[pl.ds(s * sub + r, PIECE), :] = total.astype(jnp.bfloat16)
            sy(s * per_sub + i).start()
            return carry

        lax.fori_loop(0, per_sub, one, 0)

    small[2].wait()
    wide = jnp.concatenate([wrt_ref[...].astype(jnp.float32), jnp.zeros((128 - n_experts, dim), jnp.float32)], axis=0)
    wr[...] = wide.T.astype(jnp.bfloat16)

    def total_of(p):
        s = p // per_sub
        slot = s + s // 3
        at = p - s * per_sub

        @pl.when(at == 0)
        def _():
            pair_part(slot)

        sy(p).wait_recv()
        rows = pl.ds(pl.multiple_of(at * PIECE, PIECE), PIECE)
        return keep[slot, rows, :] + drecv[slot, rows, :].astype(jnp.float32) + rbuf[piece_rows(p), :].astype(jnp.float32)

    def send_out(p):
        tbuf[piece_rows(p), :] = total_of(p).astype(jnp.bfloat16)
        ra(p).start()

    def join_in(p):
        total = total_of(p)
        ra(p).wait_recv()
        tbuf[piece_rows(p), :] = (total + abuf[piece_rows(p), :].astype(jnp.float32)).astype(jnp.bfloat16)
        rb(p).start()

    def finish(p):
        rb(p).wait_recv()
        rows = piece_rows(p)
        total = tbuf[rows, :].astype(jnp.float32) + ubuf[rows, :].astype(jnp.float32)
        out_ref[rows, :] = (h_ref[rows, :].astype(jnp.float32) + total).astype(jnp.bfloat16)
        rc(p).start()

    def pieces(rows_32):
        return [q for p in rows_32 for q in (2 * p, 2 * p + 1)]

    def line(out=(), joined=(), done=()):
        @pl.when(outer)
        def _():
            for p in pieces(out):
                send_out(p)

        @pl.when(inner)
        def _():
            for p in pieces(joined):
                join_in(p)
            for p in pieces(done):
                finish(p)

    def weights_in(which):
        for copy in which:
            copy.wait()

    pre = {0: [lambda: d1(0).wait_recv(), ids_own, lambda: weights_in(weights[:-1])],
           1: [lambda: far_in(0), lambda: d1(1).wait_recv()],
           2: [lambda: d1(2).wait_recv()],
           3: [ids_far, lambda: far_ready(0)],
           4: [lambda: far_sum(0), lambda: far_in(4), lambda: far_pair_in(2), lambda: d1(3).wait_recv()],
           5: [lambda: line((0,)), lambda: far_pair_in(3), lambda: far_ready(1)],
           6: [lambda: line((2,), (0,)), lambda: far_sum(1), lambda: far_pair_in(4), lambda: far_ready(2)],
           7: [lambda: line((4,), (2,)), lambda: far_ready(3)]}
    mid = {0: [lambda: weights_in(weights[-1:])],
           1: [lambda: far_in(1)],
           2: [lambda: far_in(2), lambda: far_pair_in(0), lambda: far_pair_in(1)],
           3: [lambda: far_in(3)],
           5: [lambda: line((1,))],
           6: [lambda: line((3,), (1,), (0,))],
           7: [lambda: far_sum(2), lambda: line((5,), (3,), (1,))]}

    def run(tasks, step):
        for k, fns in tasks.items():
            @pl.when(step == k)
            def _(fns=fns):
                for fn in fns:
                    fn()

    def chosen_of(tile):
        expert = lax.broadcasted_iota(jnp.int32, (n_experts, sub), 0)
        hit = jnp.zeros((n_experts, sub), jnp.float32)
        for j in range(tile.shape[0]):
            hit = jnp.where(tile[j:j + 1, :] == expert, 1.0, hit)
        return jnp.concatenate([hit, jnp.zeros((128 - n_experts, sub), jnp.float32)], axis=0).T

    @pl.loop(0, 2 * N_SUB)
    def _(step):
        run(pre, step)
        x = v.at[step]
        logits = jnp.dot(x[...], wr[...], preferred_element_type=jnp.float32)
        lane = lax.broadcasted_iota(jnp.int32, logits.shape, 1)
        logits = jnp.where(lane < n_experts, logits, -jnp.inf)
        raised = jnp.exp(logits - jnp.max(logits, axis=-1, keepdims=True))
        prob = raised / jnp.sum(raised, axis=-1, keepdims=True)
        chosen = jnp.concatenate([chosen_of(ids_slot[step, 0]), chosen_of(ids_slot[step, 1])], axis=0)
        gates = pltpu.roll(prob * chosen, (128 - ep * local_exp) % 128, axis=1)
        for e in range(local_exp):
            gu = jnp.dot(x[...], wgu[e], preferred_element_type=jnp.float32)
            a = (jax.nn.silu(gu[:, :width]) * gu[:, width:]).astype(jnp.bfloat16).astype(jnp.float32)
            act[:, e * width:(e + 1) * width] = (a * gates[:, e:e + 1]).astype(jnp.bfloat16)
        run(mid, step)
        for n in range(dim // COLS):
            part = jnp.dot(act[...], wd[:, n * COLS:(n + 1) * COLS], preferred_element_type=jnp.float32)
            keep[step, :, n * COLS:(n + 1) * COLS] = part[:sub]
            dsend[step, :, n * COLS:(n + 1) * COLS] = part[sub:].astype(jnp.bfloat16)
        for n in range(dim // COLS):
            pd(step, n).start()

    @pl.when(outer)
    def _():
        @pl.loop(12, n_piece)
        def _(p):
            @pl.when(p == 16)
            def _():
                far_sum(3)

            send_out(p)

        @pl.loop(0, n_piece)
        def _(p):
            rc(p).wait_recv()

    @pl.when(inner)
    def _():
        finish(4)

        @pl.loop(8, n_piece)
        def _(p):
            @pl.when(p == 10)
            def _():
                far_sum(3)

            join_in(p)
            finish(p - 3)

        finish(n_piece - 3)
        finish(n_piece - 2)
        finish(n_piece - 1)

    for k in range(3):
        ids_copy(k).wait_send()
    for s in range(N_SUB):
        d1(s).wait_send()
    for u in range(len(UNITS)):
        dy(u).wait_send()
        dz(u, side).wait_send()
        dd(u, 0).wait_send()
        dd(u, 1).wait_send()

    @pl.loop(0, 2 * N_SUB)
    def _(slot):
        for n in range(dim // COLS):
            pd(slot, n).wait_send()

    @pl.loop(0, n_piece)
    def _(p):
        sy(p).wait_send()

        @pl.when(outer)
        def _():
            ra(p).wait_send()

        @pl.when(inner)
        def _():
            rb(p).wait_send()
            rc(p).wait_send()


def solution(mesh):
    def per_device(hidden, expert_ids, norm_w, router_w, w_gate, w_up, w_down):
        tok, dim = hidden.shape
        top_k = expert_ids.shape[1]
        local_exp, _, width = w_gate.shape
        sub = tok // N_SUB
        n_piece = tok // PIECE
        ids_t = expert_ids.reshape(N_SUB, sub, top_k).transpose(0, 2, 1)
        bf, f32 = jnp.bfloat16, jnp.float32
        vmem = pl.BlockSpec(memory_space=pltpu.VMEM)
        hbm = pl.BlockSpec(memory_space=pltpu.HBM)
        dma = pltpu.SemaphoreType.DMA
        scratch = [
            pltpu.VMEM((N_SUB, top_k, sub), jnp.int32),
            pltpu.VMEM((dim,), bf),
            pltpu.VMEM((router_w.shape[1], dim), bf),
            pltpu.VMEM((tok, dim), bf),
            pltpu.VMEM((dim, 128), bf),
            pltpu.VMEM((2 * N_SUB, 2 * sub, dim), bf),
            pltpu.VMEM((local_exp, dim, 2 * width), bf),
            pltpu.VMEM((local_exp * width, dim), bf),
            pltpu.VMEM((2 * sub, local_exp * width), bf),
            pltpu.VMEM((2 * N_SUB, sub, dim), f32),
            pltpu.VMEM((2 * N_SUB, sub, dim), bf),
            pltpu.VMEM((2 * N_SUB, sub, dim), bf),
            pltpu.VMEM((tok, dim), bf),
            pltpu.VMEM((tok, dim), bf),
            pltpu.VMEM((tok, dim), bf),
            pltpu.VMEM((tok, dim), bf),
            pltpu.VMEM((tok, dim), bf),
            pltpu.VMEM((3, N_SUB, top_k, sub), jnp.int32),
            pltpu.VMEM((2 * N_SUB, 2, top_k, sub), jnp.int32),
            dma((N_SUB + 3,)),
            dma((2 * local_exp + 1,)),
            dma((3,)), dma((3,)),
            dma((N_SUB,)), dma((N_SUB,)),
            dma((len(UNITS),)), dma((len(UNITS),)),
            dma((len(UNITS),)), dma((len(UNITS),)),
            dma((2 * len(UNITS),)), dma((2 * len(UNITS),)),
            dma((2 * N_SUB * dim // COLS,)), dma((2 * N_SUB * dim // COLS,)),
            dma((n_piece,)), dma((n_piece,)),
            dma((n_piece,)), dma((n_piece,)),
            dma((n_piece,)), dma((n_piece,)),
            dma((n_piece,)), dma((n_piece,)),
        ]
        return pl.pallas_call(
            body,
            out_shape=jax.ShapeDtypeStruct((tok, dim), bf),
            in_specs=[hbm] * 7,
            out_specs=vmem,
            scratch_shapes=scratch,
            compiler_params=pltpu.CompilerParams(collective_id=0, has_side_effects=True, vmem_limit_bytes=53_000_000),
            name="moe_layer",
        )(*[pltpu.with_memory_space_constraint(x, pltpu.HBM) for x in (ids_t, hidden, norm_w, router_w.T, w_gate, w_up, w_down.reshape(local_exp * width, dim))])

    token_spec = P(("dp", "ep"), None)
    return jax.shard_map(per_device, mesh=mesh, in_specs=(token_spec, token_spec, P(None), P(None, None), P("ep", None, "tp"), P("ep", None, "tp"), P("ep", "tp", None)), out_specs=token_spec, check_vma=False)
```

```python
import jax
import jax.numpy as jnp
from jax import lax
from jax.experimental import pallas as pl
from jax.experimental.pallas import tpu as pltpu
from jax.sharding import PartitionSpec as P

NORM_EPS = 1e-6
MESH = pl.DeviceIdType.MESH
N_BLK = 8
PIECE = 16
COLS = 512
JOBS = (
    (("own", 0), ("own", 1)),
    (("own", 2), ("own", 3)),
    (("far", 0), ("own", 4)),
    (("far", 1), ("own", 5)),
    (("far", 2), ("far", 3)),
    (("far", 4), ("far", 5)),
    (("own", 6), ("own", 7)),
    (("far", 6), ("far", 7)),
)
PLACE = {block: (slot, k) for slot, job in enumerate(JOBS) for k, block in enumerate(job)}
WHOLE = 6
UNITS = ((0, 0, 16), (0, 16, 16)) + tuple((b, 0, 32) for b in range(1, WHOLE))


def body(ids_hbm, h_hbm, nw_hbm, wrt_hbm, wg_hbm, wu_hbm, wd_hbm, out_ref,
         ids_ref, nw_ref, wrt_ref, h_ref, wr, v, wgu, wd, act, keep, dsend, drecv, sbuf, rbuf, tbuf, abuf, ubuf, ids_all, ids_slot,
         h_sem, w_sem, ids_s, ids_r, d1_s, d1_r, dy_s, dy_r, dz_s, dz_r, dyw_s, dyw_r, dzw_s, dzw_r, dd_s, dd_r, pd_s, pd_r,
         sy_s, sy_r, rac_s, rac_r, rb_s, rb_r):
    tok, dim = h_ref.shape
    n_experts = wrt_ref.shape[0]
    local_exp, _, width = wg_hbm.shape
    blk = tok // N_BLK
    half = blk // 2
    mine = 2 * blk
    n_job = len(JOBS)
    n_piece = tok // PIECE
    per_blk = blk // PIECE
    ep = lax.axis_index("ep")
    z = lax.axis_index("tp")
    core, y = ep % 2, ep // 2
    ep_pair = 2 * y + 1 - core
    ep_far = 2 * (1 - y) + core
    ep_diag = 2 * (1 - y) + 1 - core
    side = z % 2
    z_pair = z + 1 - 2 * side
    z_mirror = 3 - z
    inner = jnp.logical_or(z == 1, z == 2)
    outer = jnp.logical_or(z == 0, z == 3)

    def remote(src, dst, ssem, rsem, **where):
        return pltpu.make_async_remote_copy(src_ref=src, dst_ref=dst, send_sem=ssem, recv_sem=rsem, device_id=where, device_id_type=MESH)

    def weight_copies():
        copies = []
        for e in range(local_exp):
            copies.append(pltpu.make_async_copy(wg_hbm.at[e], wgu.at[e, :, pl.ds(0, width)], w_sem.at[0]))
            copies.append(pltpu.make_async_copy(wu_hbm.at[e], wgu.at[e, :, pl.ds(width, width)], w_sem.at[0]))
        copies.append(pltpu.make_async_copy(wd_hbm, wd, w_sem.at[1]))
        return copies

    def h_copy(k):
        rows = pl.ds(k * mine, mine)
        return pltpu.make_async_copy(h_hbm.at[rows], h_ref.at[rows], h_sem.at[k])

    n_h = tok // mine
    small = [pltpu.make_async_copy(src, dst, h_sem.at[n_h + k]) for k, (src, dst) in enumerate(((nw_hbm, nw_ref), (ids_hbm, ids_ref), (wrt_hbm, wrt_ref)))]
    h_copy(0).start()
    for copy in small:
        copy.start()
    for k in range(1, n_h):
        h_copy(k).start()
    barrier = pltpu.get_barrier_semaphore()
    for where in ({"ep": ep_pair}, {"ep": ep_far}, {"ep": ep_diag}, {"tp": z_pair}, {"tp": z_mirror}):
        pl.semaphore_signal(barrier, inc=1, device_id=where, device_id_type=MESH)
    for copy in weight_copies():
        copy.start()

    small[0].wait()
    scale = nw_ref[...].astype(jnp.float32).reshape(1, dim)

    def norm_block(b):
        slot, k = PLACE["own", b]
        if b % 2 == 0:
            h_copy(b // 2).wait()

        def group(i, carry):
            r = pl.multiple_of(i * 16, 16)
            x = h_ref[pl.ds(b * blk + r, 16), :].astype(jnp.float32)
            ms = jnp.mean(x * x, axis=-1, keepdims=True)
            v[slot, pl.ds(k * blk + r, 16), :] = (x * lax.rsqrt(ms + NORM_EPS) * scale).astype(jnp.bfloat16)
            return carry

        lax.fori_loop(0, blk // 16, group, 0, unroll=True)

    def unit(kind, u, which, base=0):
        b, first, rows = UNITS[u]
        slot, k = PLACE[kind, b]
        return v.at[slot, pl.ds(pl.multiple_of(base + k * blk + which * half + first, 16), rows)]

    def block(kind, b, base=0):
        slot, k = PLACE[kind, b]
        return v.at[slot, pl.ds(base + k * blk, blk)]

    def ids_copy(k):
        ep_to = (ep_pair, ep_far, ep_diag)[k]
        return remote(ids_ref, ids_all.at[k], ids_s, ids_r.at[k], ep=ep_to)

    def d1(b):
        return remote(block("own", b), block("own", b, mine), d1_s, d1_r.at[PLACE["own", b][0]], ep=ep_pair)

    def dy(u):
        return remote(unit("own", u, side), unit("far", u, side), dy_s, dy_r.at[u], ep=ep_far)

    def dz(u, which):
        return remote(unit("far", u, which), unit("far", u, which), dz_s, dz_r.at[u], tp=z_pair)

    def dd(u, which):
        return remote(unit("far", u, which), unit("far", u, which, mine), dd_s, dd_r.at[UNITS[u][0]], ep=ep_pair)

    def dy_whole(b):
        return remote(block("own", b), block("far", b), dyw_s, dyw_r.at[b - WHOLE], ep=ep_far)

    def dz_whole(b):
        return remote(block("far", b), block("far", b), dzw_s, dzw_r.at[b - WHOLE], tp=z_pair)

    def dd_whole(b):
        return remote(block("far", b), block("far", b, mine), dd_s, dd_r.at[b], ep=ep_pair)

    def pd(slot, n):
        cols = pl.ds(n * COLS, COLS)
        return remote(dsend.at[slot, :, cols], drecv.at[slot, :, cols], pd_s, pd_r.at[slot], ep=ep_pair)

    def piece_rows(p):
        return pl.ds(pl.multiple_of(p * PIECE, PIECE), PIECE)

    def sy(p):
        return remote(sbuf.at[piece_rows(p)], rbuf.at[piece_rows(p)], sy_s, sy_r.at[p], ep=ep_far)

    def ra(p):
        return remote(tbuf.at[piece_rows(p)], abuf.at[piece_rows(p)], rac_s, rac_r.at[p], tp=z_pair)

    def rb(p):
        return remote(tbuf.at[piece_rows(p)], ubuf.at[piece_rows(p)], rb_s, rb_r.at[p], tp=z_mirror)

    def rc(p):
        return remote(out_ref.at[piece_rows(p)], out_ref.at[piece_rows(p)], rac_s, rac_r.at[p], tp=z_pair)

    for b in range(N_BLK):
        norm_block(b)
        if b == 0:
            pl.semaphore_wait(barrier, 5)
        for u, (of, _, _) in enumerate(UNITS):
            if of == b:
                dy(u).start()
        if b >= WHOLE:
            @pl.when(inner)
            def _(b=b):
                dy_whole(b).start()
        d1(b).start()
        if b == 0:
            small[1].wait()
            for k in range(3):
                ids_copy(k).start()

    def own_in(slot):
        of_job = [b for kind, b in JOBS[slot] if kind == "own"]
        rows = v.at[slot, pl.ds(mine + PLACE["own", of_job[0]][1] * blk, len(of_job) * blk)]
        remote(rows, rows, d1_s, d1_r.at[slot], ep=ep_pair).wait_recv()

    def far_in(u):
        dy(u).wait_recv()
        dz(u, side).start()
        dd(u, side).start()

    def far_pair_in(u):
        dz(u, 1 - side).wait_recv()
        dd(u, 1 - side).start()

    def whole_in(b):
        @pl.when(inner)
        def _():
            dy_whole(b).wait_recv()
            dz_whole(b).start()
            dd_whole(b).start()

    def whole_pair_in(b):
        @pl.when(outer)
        def _():
            dz_whole(b).wait_recv()
            dd_whole(b).start()

    def far_ready(*blocks):
        for b in blocks:
            remote(block("far", b), block("far", b, mine), dd_s, dd_r.at[b], ep=ep_pair).wait_recv()

    def ids_own():
        ids_copy(0).wait_recv()
        for b in range(N_BLK):
            slot, k = PLACE["own", b]
            lanes, at = slice(b % 2 * blk, (b % 2 + 1) * blk), slice(k * blk, (k + 1) * blk)
            ids_slot[slot, 0, :, at] = ids_ref[b // 2, :, lanes]
            ids_slot[slot, 1, :, at] = ids_all[0, b // 2, :, lanes]

    def ids_far():
        ids_copy(1).wait_recv()
        ids_copy(2).wait_recv()
        for b in range(N_BLK):
            slot, k = PLACE["far", b]
            lanes, at = slice(b % 2 * blk, (b % 2 + 1) * blk), slice(k * blk, (k + 1) * blk)
            ids_slot[slot, 0, :, at] = ids_all[1, b // 2, :, lanes]
            ids_slot[slot, 1, :, at] = ids_all[2, b // 2, :, lanes]

    def pair_part(slot):
        remote(dsend.at[slot], drecv.at[slot], pd_s, pd_r.at[slot], ep=ep_pair).wait_recv()

    def far_sum(b):
        slot, k = PLACE["far", b]

        def one(i, carry):
            rows = pl.ds(pl.multiple_of(k * blk + i * PIECE, PIECE), PIECE)
            total = keep[slot, rows, :] + drecv[slot, rows, :].astype(jnp.float32)
            sbuf[piece_rows(b * per_blk + i), :] = total.astype(jnp.bfloat16)
            sy(b * per_blk + i).start()
            return carry

        lax.fori_loop(0, per_blk, one, 0)

    small[2].wait()
    wide = jnp.concatenate([wrt_ref[...].astype(jnp.float32), jnp.zeros((128 - n_experts, dim), jnp.float32)], axis=0)
    wr[...] = wide.T.astype(jnp.bfloat16)

    def total_of(b, i):
        slot, k = PLACE["own", b]
        p = b * per_blk + i
        sy(p).wait_recv()
        rows = pl.ds(pl.multiple_of(k * blk + i * PIECE, PIECE), PIECE)
        return keep[slot, rows, :] + drecv[slot, rows, :].astype(jnp.float32) + rbuf[piece_rows(p), :].astype(jnp.float32)

    def send_out(b, i):
        p = b * per_blk + i
        tbuf[piece_rows(p), :] = total_of(b, i).astype(jnp.bfloat16)
        ra(p).start()

    def join_in(b, i):
        p = b * per_blk + i
        total = total_of(b, i)
        ra(p).wait_recv()
        tbuf[piece_rows(p), :] = (total + abuf[piece_rows(p), :].astype(jnp.float32)).astype(jnp.bfloat16)
        rb(p).start()

    def finish(p):
        rb(p).wait_recv()
        rows = piece_rows(p)
        total = tbuf[rows, :].astype(jnp.float32) + ubuf[rows, :].astype(jnp.float32)
        out_ref[rows, :] = (h_ref[rows, :].astype(jnp.float32) + total).astype(jnp.bfloat16)
        rc(p).start()

    def line(out=(), joined=(), done=()):
        @pl.when(outer)
        def _():
            for p in out:
                send_out(*divmod(p, per_blk))

        @pl.when(inner)
        def _():
            for p in joined:
                join_in(*divmod(p, per_blk))
            for p in done:
                finish(p)

    def weights_in(ref, k):
        pltpu.make_async_copy(ref, ref, w_sem.at[k]).wait()

    def each(fn, *args):
        return lambda: fn(*args)

    pre = {0: [each(own_in, 0), ids_own, each(weights_in, wgu, 0)],
           1: [each(far_in, 1), each(own_in, 1)],
           2: [ids_far, each(own_in, 2), each(far_in, 3), each(far_ready, 0)],
           3: [each(far_in, 5), each(pair_part, 2), each(far_sum, 0), each(far_pair_in, 3),
               each(own_in, 3), each(far_ready, 1), each(pair_part, 0), each(pair_part, 1)],
           4: [each(whole_in, 6), each(far_pair_in, 5), each(line, (0,)), each(far_ready, 2, 3)],
           5: [each(line, (), (0,)), each(whole_in, 7), each(far_ready, 4, 5)],
           6: [each(line, (6,), (3,), (0,)), each(whole_pair_in, 6), each(own_in, 6)],
           7: [each(line, (10, 11), (6, 7), (3,)), each(far_ready, 6, 7)]}
    early = {2: [each(far_in, 4)],
             3: [each(far_in, 6), each(far_pair_in, 4)],
             4: [each(pair_part, 3), each(far_sum, 1), each(line, (1, 2))],
             5: [each(pair_part, 4), each(far_sum, 2), each(far_sum, 3), each(line, (4,), (1,))],
             6: [each(pair_part, 5), each(far_sum, 4), each(far_sum, 5), each(line, (7, 8), (4,), (1,))],
             7: [each(pair_part, 6), each(line, (12,), (8,), (4,))]}
    mid = {0: [each(weights_in, wd, 1), each(far_in, 0)],
           1: [each(far_in, 2), each(far_pair_in, 0), each(far_pair_in, 1)],
           2: [each(far_pair_in, 2)],
           4: [each(line, (3,)), each(far_pair_in, 6)],
           5: [each(line, (5,), (2,))],
           6: [each(line, (9,), (5,), (2,)), each(whole_pair_in, 7)],
           7: [each(line, (13, 14), (9, 10), (5, 6))]}
    out_from, join_from, lag = 15, 11, 4

    def run(tasks, step):
        for k, fns in tasks.items():
            @pl.when(step == k)
            def _(fns=fns):
                for fn in fns:
                    fn()

    def chosen_of(tile):
        expert = lax.broadcasted_iota(jnp.int32, (n_experts, mine), 0)
        hit = jnp.zeros((n_experts, mine), jnp.float32)
        for j in range(tile.shape[0]):
            hit = jnp.where(tile[j:j + 1, :] == expert, 1.0, hit)
        return jnp.concatenate([hit, jnp.zeros((128 - n_experts, mine), jnp.float32)], axis=0).T

    @pl.loop(0, n_job)
    def _(step):
        run(pre, step)
        x = v.at[step]
        logits = jnp.dot(x[...], wr[...], preferred_element_type=jnp.float32)
        lane = lax.broadcasted_iota(jnp.int32, logits.shape, 1)
        logits = jnp.where(lane < n_experts, logits, -jnp.inf)
        raised = jnp.exp(logits - jnp.max(logits, axis=-1, keepdims=True))
        prob = raised / jnp.sum(raised, axis=-1, keepdims=True)
        chosen = jnp.concatenate([chosen_of(ids_slot[step, 0]), chosen_of(ids_slot[step, 1])], axis=0)
        gates = pltpu.roll(prob * chosen, (128 - ep * local_exp) % 128, axis=1)
        for e in range(local_exp):
            gu = jnp.dot(x[...], wgu[e], preferred_element_type=jnp.float32)
            if e == local_exp // 2:
                run(early, step)
            a = (jax.nn.silu(gu[:, :width]) * gu[:, width:]).astype(jnp.bfloat16).astype(jnp.float32)
            act[:, e * width:(e + 1) * width] = (a * gates[:, e:e + 1]).astype(jnp.bfloat16)
        run(mid, step)
        for n in range(dim // COLS):
            part = jnp.dot(act[...], wd[:, n * COLS:(n + 1) * COLS], preferred_element_type=jnp.float32)
            keep[step, :, n * COLS:(n + 1) * COLS] = part[:mine]
            dsend[step, :, n * COLS:(n + 1) * COLS] = part[mine:].astype(jnp.bfloat16)
        for n in range(dim // COLS):
            pd(step, n).start()

    @pl.when(outer)
    def _():
        for b in range(out_from // per_blk, N_BLK):
            if b == 4:
                pair_part(7)
                far_sum(6)
                far_sum(7)

            @pl.loop(max(out_from - b * per_blk, 0), per_blk)
            def _(i, b=b):
                send_out(b, i)

        @pl.loop(0, n_piece)
        def _(p):
            rc(p).wait_recv()

    @pl.when(inner)
    def _():
        for b in range(join_from // per_blk, N_BLK):
            if b == 4:
                pair_part(7)
                far_sum(6)
                far_sum(7)

            @pl.loop(max(join_from - b * per_blk, 0), per_blk)
            def _(i, b=b):
                join_in(b, i)
                finish(b * per_blk + i - lag)

        for p in range(n_piece - lag, n_piece):
            finish(p)

    remote(ids_all, ids_all, ids_s, ids_r.at[0], ep=ep_pair).wait_send()
    two, shared, whole = v.at[pl.ds(0, 2)], v.at[0, pl.ds(0, WHOLE * half)], v.at[0, pl.ds(0, (N_BLK - WHOLE) * blk)]
    remote(two, two, d1_s, d1_r.at[0], ep=ep_pair).wait_send()
    remote(shared, shared, dy_s, dy_r.at[0], ep=ep_far).wait_send()
    remote(shared, shared, dz_s, dz_r.at[0], tp=z_pair).wait_send()
    remote(two, two, dd_s, dd_r.at[0], ep=ep_pair).wait_send()
    remote(dsend, drecv, pd_s, pd_r.at[0], ep=ep_pair).wait_send()
    remote(sbuf, rbuf, sy_s, sy_r.at[0], ep=ep_far).wait_send()

    @pl.when(outer)
    def _():
        remote(tbuf, abuf, rac_s, rac_r.at[0], tp=z_pair).wait_send()

    @pl.when(inner)
    def _():
        remote(whole, whole, dyw_s, dyw_r.at[0], ep=ep_far).wait_send()
        remote(whole, whole, dzw_s, dzw_r.at[0], tp=z_pair).wait_send()
        remote(tbuf, ubuf, rb_s, rb_r.at[0], tp=z_mirror).wait_send()
        remote(out_ref, out_ref, rac_s, rac_r.at[0], tp=z_pair).wait_send()


def solution(mesh):
    def per_device(hidden, expert_ids, norm_w, router_w, w_gate, w_up, w_down):
        tok, dim = hidden.shape
        top_k = expert_ids.shape[1]
        local_exp, _, width = w_gate.shape
        blk = tok // N_BLK
        n_job = len(JOBS)
        n_piece = tok // PIECE
        ids_t = expert_ids.reshape(N_BLK // 2, 2 * blk, top_k).transpose(0, 2, 1)
        bf, f32 = jnp.bfloat16, jnp.float32
        dma = pltpu.SemaphoreType.DMA
        scratch = [
            pltpu.VMEM((N_BLK // 2, top_k, 2 * blk), jnp.int32),
            pltpu.VMEM((dim,), bf),
            pltpu.VMEM((router_w.shape[1], dim), bf),
            pltpu.VMEM((tok, dim), bf),
            pltpu.VMEM((dim, 128), bf),
            pltpu.VMEM((n_job, 4 * blk, dim), bf),
            pltpu.VMEM((local_exp, dim, 2 * width), bf),
            pltpu.VMEM((local_exp * width, dim), bf),
            pltpu.VMEM((4 * blk, local_exp * width), bf),
            pltpu.VMEM((n_job, 2 * blk, dim), f32),
            pltpu.VMEM((n_job, 2 * blk, dim), bf),
            pltpu.VMEM((n_job, 2 * blk, dim), bf),
            pltpu.VMEM((tok, dim), bf),
            pltpu.VMEM((tok, dim), bf),
            pltpu.VMEM((tok, dim), bf),
            pltpu.VMEM((tok, dim), bf),
            pltpu.VMEM((tok, dim), bf),
            pltpu.VMEM((3, N_BLK // 2, top_k, 2 * blk), jnp.int32),
            pltpu.VMEM((n_job, 2, top_k, 2 * blk), jnp.int32),
            dma((tok // (2 * blk) + 3,)),
            dma((2,)),
            dma, dma((3,)),
            dma, dma((n_job,)),
            dma, dma((len(UNITS),)),
            dma, dma((len(UNITS),)),
            dma, dma((N_BLK - WHOLE,)),
            dma, dma((N_BLK - WHOLE,)),
            dma, dma((N_BLK,)),
            dma, dma((n_job,)),
            dma, dma((n_piece,)),
            dma, dma((n_piece,)),
            dma, dma((n_piece,)),
        ]
        operands = (ids_t, hidden, norm_w, router_w.T, w_gate, w_up, w_down.reshape(local_exp * width, dim))
        return pl.pallas_call(
            body,
            out_shape=jax.ShapeDtypeStruct((tok, dim), bf),
            in_specs=[pl.BlockSpec(memory_space=pltpu.HBM)] * len(operands),
            out_specs=pl.BlockSpec(memory_space=pltpu.VMEM),
            scratch_shapes=scratch,
            compiler_params=pltpu.CompilerParams(collective_id=0, has_side_effects=True, vmem_limit_bytes=53_000_000),
            name="moe_layer",
        )(*[pltpu.with_memory_space_constraint(x, pltpu.HBM) for x in operands])

    token_spec = P(("dp", "ep"), None)
    return jax.shard_map(per_device, mesh=mesh, in_specs=(token_spec, token_spec, P(None), P(None, None), P("ep", None, "tp"), P("ep", None, "tp"), P("ep", "tp", None)), out_specs=token_spec, check_vma=False)
```

```python
import jax
import jax.numpy as jnp
from jax import lax
from jax.experimental import pallas as pl
from jax.experimental.pallas import tpu as pltpu
from jax.sharding import PartitionSpec as P

NORM_EPS = 1e-6
MESH = pl.DeviceIdType.MESH
N_BLK = 8
PIECE = 16
COLS = 512
JOBS = (
    (("own", 0), ("own", 1)),
    (("own", 2), ("own", 3)),
    (("far", 0), ("own", 4)),
    (("far", 1), ("own", 5)),
    (("far", 2), ("far", 3)),
    (("far", 4), ("far", 5)),
    (("own", 6), ("own", 7)),
    (("far", 6), ("far", 7)),
)
PLACE = {block: (slot, k) for slot, job in enumerate(JOBS) for k, block in enumerate(job)}
WHOLE = 6
UNITS = ((0, 0, 16), (0, 16, 16)) + tuple((b, 0, 32) for b in range(1, WHOLE))


def body(ids_hbm, h_hbm, nw_hbm, wrt_hbm, wg_hbm, wu_hbm, wd_hbm, out_ref,
         ids_ref, nw_ref, wrt_ref, h_ref, wr, v, wgu, wd, act, keep, dsend, drecv, sbuf, rbuf, tbuf, abuf, ubuf, ids_all, ids_slot,
         h_sem, w_sem, ids_s, ids_r, d1_s, d1_r, dy_s, dy_r, dz_s, dz_r, dyw_s, dyw_r, dzw_s, dzw_r, dd_s, dd_r, pd_s, pd_r,
         sy_s, sy_r, rac_s, rac_r, rb_s, rb_r):
    tok, dim = h_ref.shape
    n_experts = wrt_ref.shape[0]
    local_exp, _, width = wg_hbm.shape
    blk = tok // N_BLK
    half = blk // 2
    mine = 2 * blk
    n_job = len(JOBS)
    n_piece = tok // PIECE
    per_blk = blk // PIECE
    ep = lax.axis_index("ep")
    z = lax.axis_index("tp")
    core, y = ep % 2, ep // 2
    ep_pair = 2 * y + 1 - core
    ep_far = 2 * (1 - y) + core
    ep_diag = 2 * (1 - y) + 1 - core
    side = z % 2
    z_pair = z + 1 - 2 * side
    z_mirror = 3 - z
    inner = jnp.logical_or(z == 1, z == 2)
    outer = jnp.logical_or(z == 0, z == 3)

    def remote(src, dst, ssem, rsem, **where):
        return pltpu.make_async_remote_copy(src_ref=src, dst_ref=dst, send_sem=ssem, recv_sem=rsem, device_id=where, device_id_type=MESH)

    first_exp = local_exp // 2 + 1

    def weight_copies():
        copies = []
        for e in range(local_exp):
            copies.append(pltpu.make_async_copy(wg_hbm.at[e], wgu.at[e, :, pl.ds(0, width)], w_sem.at[e // first_exp]))
            copies.append(pltpu.make_async_copy(wu_hbm.at[e], wgu.at[e, :, pl.ds(width, width)], w_sem.at[e // first_exp]))
        copies.append(pltpu.make_async_copy(wd_hbm, wd, w_sem.at[2]))
        return copies

    def h_copy(k):
        rows = pl.ds(k * mine, mine)
        return pltpu.make_async_copy(h_hbm.at[rows], h_ref.at[rows], h_sem.at[k])

    n_h = tok // mine
    small = [pltpu.make_async_copy(src, dst, h_sem.at[n_h + k]) for k, (src, dst) in enumerate(((nw_hbm, nw_ref), (ids_hbm, ids_ref), (wrt_hbm, wrt_ref)))]
    h_copy(0).start()
    for copy in small:
        copy.start()
    for k in range(1, n_h):
        h_copy(k).start()
    barrier = pltpu.get_barrier_semaphore()
    for where in ({"ep": ep_pair}, {"ep": ep_far}, {"ep": ep_diag}, {"tp": z_pair}):
        pl.semaphore_signal(barrier, inc=1, device_id=where, device_id_type=MESH)

    @pl.when(inner)
    def _():
        pl.semaphore_signal(barrier, inc=1, device_id={"tp": z_mirror}, device_id_type=MESH)

    for copy in weight_copies():
        copy.start()

    small[0].wait()
    scale = nw_ref[...].astype(jnp.float32).reshape(1, dim)

    def norm_block(b):
        slot, k = PLACE["own", b]
        if b % 2 == 0:
            h_copy(b // 2).wait()

        def group(i, carry):
            r = pl.multiple_of(i * 16, 16)
            x = h_ref[pl.ds(b * blk + r, 16), :].astype(jnp.float32)
            ms = jnp.mean(x * x, axis=-1, keepdims=True)
            v[slot, pl.ds(k * blk + r, 16), :] = (x * lax.rsqrt(ms + NORM_EPS) * scale).astype(jnp.bfloat16)
            return carry

        lax.fori_loop(0, blk // 16, group, 0, unroll=True)

    def unit(kind, u, which, base=0):
        b, first, rows = UNITS[u]
        slot, k = PLACE[kind, b]
        return v.at[slot, pl.ds(pl.multiple_of(base + k * blk + which * half + first, 16), rows)]

    def block(kind, b, base=0):
        slot, k = PLACE[kind, b]
        return v.at[slot, pl.ds(base + k * blk, blk)]

    def ids_copy(k):
        ep_to = (ep_pair, ep_far, ep_diag)[k]
        return remote(ids_ref, ids_all.at[k], ids_s, ids_r.at[k], ep=ep_to)

    def d1(b):
        return remote(block("own", b), block("own", b, mine), d1_s, d1_r.at[PLACE["own", b][0]], ep=ep_pair)

    def dy(u):
        return remote(unit("own", u, side), unit("far", u, side), dy_s, dy_r.at[u], ep=ep_far)

    def dz(u, which):
        return remote(unit("far", u, which), unit("far", u, which), dz_s, dz_r.at[u], tp=z_pair)

    def dd(u, which):
        return remote(unit("far", u, which), unit("far", u, which, mine), dd_s, dd_r.at[UNITS[u][0]], ep=ep_pair)

    def dy_whole(b):
        return remote(block("own", b), block("far", b), dyw_s, dyw_r.at[b - WHOLE], ep=ep_far)

    def dz_whole(b):
        return remote(block("far", b), block("far", b), dzw_s, dzw_r.at[b - WHOLE], tp=z_pair)

    def dd_whole(b):
        return remote(block("far", b), block("far", b, mine), dd_s, dd_r.at[b], ep=ep_pair)

    def pd(slot, n):
        cols = pl.ds(n * COLS, COLS)
        return remote(dsend.at[slot, :, cols], drecv.at[slot, :, cols], pd_s, pd_r.at[slot], ep=ep_pair)

    def piece_rows(p):
        return pl.ds(pl.multiple_of(p * PIECE, PIECE), PIECE)

    def sy(p):
        return remote(sbuf.at[piece_rows(p)], rbuf.at[piece_rows(p)], sy_s, sy_r.at[p], ep=ep_far)

    def ra(p):
        return remote(tbuf.at[piece_rows(p)], abuf.at[piece_rows(p)], rac_s, rac_r.at[p], tp=z_pair)

    def rb(p):
        return remote(tbuf.at[piece_rows(p)], ubuf.at[piece_rows(p)], rb_s, rb_r.at[p], tp=z_mirror)

    def rc(p):
        return remote(out_ref.at[piece_rows(p)], out_ref.at[piece_rows(p)], rac_s, rac_r.at[p], tp=z_pair)

    for b in range(N_BLK):
        norm_block(b)
        if b == 0:
            pl.semaphore_wait(barrier, jnp.where(inner, 5, 4))
        for u, (of, _, _) in enumerate(UNITS):
            if of == b:
                dy(u).start()
        if b >= WHOLE:
            @pl.when(inner)
            def _(b=b):
                dy_whole(b).start()
        d1(b).start()
        if b == 0:
            small[1].wait()
            for k in range(3):
                ids_copy(k).start()

    def own_in(slot):
        of_job = [b for kind, b in JOBS[slot] if kind == "own"]
        rows = v.at[slot, pl.ds(mine + PLACE["own", of_job[0]][1] * blk, len(of_job) * blk)]
        remote(rows, rows, d1_s, d1_r.at[slot], ep=ep_pair).wait_recv()

    def far_in(u):
        dy(u).wait_recv()
        dz(u, side).start()
        dd(u, side).start()

    def far_pair_in(u):
        dz(u, 1 - side).wait_recv()
        dd(u, 1 - side).start()

    def whole_in(b):
        @pl.when(inner)
        def _():
            dy_whole(b).wait_recv()
            dz_whole(b).start()
            dd_whole(b).start()

    def whole_pair_in(b):
        @pl.when(outer)
        def _():
            dz_whole(b).wait_recv()
            dd_whole(b).start()

    def far_ready(*blocks):
        for b in blocks:
            remote(block("far", b), block("far", b, mine), dd_s, dd_r.at[b], ep=ep_pair).wait_recv()

    def ids_own():
        ids_copy(0).wait_recv()
        for b in range(N_BLK):
            slot, k = PLACE["own", b]
            lanes, at = slice(b % 2 * blk, (b % 2 + 1) * blk), slice(k * blk, (k + 1) * blk)
            ids_slot[slot, 0, :, at] = ids_ref[b // 2, :, lanes]
            ids_slot[slot, 1, :, at] = ids_all[0, b // 2, :, lanes]

    def ids_far():
        ids_copy(1).wait_recv()
        ids_copy(2).wait_recv()
        for b in range(N_BLK):
            slot, k = PLACE["far", b]
            lanes, at = slice(b % 2 * blk, (b % 2 + 1) * blk), slice(k * blk, (k + 1) * blk)
            ids_slot[slot, 0, :, at] = ids_all[1, b // 2, :, lanes]
            ids_slot[slot, 1, :, at] = ids_all[2, b // 2, :, lanes]

    def pair_part(slot):
        remote(dsend.at[slot], drecv.at[slot], pd_s, pd_r.at[slot], ep=ep_pair).wait_recv()

    def far_sum(b):
        slot, k = PLACE["far", b]

        def one(i, carry):
            rows = pl.ds(pl.multiple_of(k * blk + i * PIECE, PIECE), PIECE)
            total = keep[slot, rows, :] + drecv[slot, rows, :].astype(jnp.float32)
            sbuf[piece_rows(b * per_blk + i), :] = total.astype(jnp.bfloat16)
            sy(b * per_blk + i).start()
            return carry

        lax.fori_loop(0, per_blk, one, 0)

    small[2].wait()
    wide = jnp.concatenate([wrt_ref[...].astype(jnp.float32), jnp.zeros((128 - n_experts, dim), jnp.float32)], axis=0)
    wr[...] = wide.T.astype(jnp.bfloat16)

    def total_of(b, i):
        slot, k = PLACE["own", b]
        p = b * per_blk + i
        sy(p).wait_recv()
        rows = pl.ds(pl.multiple_of(k * blk + i * PIECE, PIECE), PIECE)
        return keep[slot, rows, :] + drecv[slot, rows, :].astype(jnp.float32) + rbuf[piece_rows(p), :].astype(jnp.float32)

    def send_out(b, i):
        p = b * per_blk + i
        tbuf[piece_rows(p), :] = total_of(b, i).astype(jnp.bfloat16)
        ra(p).start()

    def join_in(b, i):
        p = b * per_blk + i
        total = total_of(b, i)
        ra(p).wait_recv()
        tbuf[piece_rows(p), :] = (total + abuf[piece_rows(p), :].astype(jnp.float32)).astype(jnp.bfloat16)
        rb(p).start()

    def finish(p):
        rb(p).wait_recv()
        rows = piece_rows(p)
        total = tbuf[rows, :].astype(jnp.float32) + ubuf[rows, :].astype(jnp.float32)
        out_ref[rows, :] = (h_ref[rows, :].astype(jnp.float32) + total).astype(jnp.bfloat16)
        rc(p).start()

    def line(out=(), joined=(), done=()):
        @pl.when(outer)
        def _():
            for p in out:
                send_out(*divmod(p, per_blk))

        @pl.when(inner)
        def _():
            for p in joined:
                join_in(*divmod(p, per_blk))
            for p in done:
                finish(p)

    def weights_in(ref, k):
        pltpu.make_async_copy(ref, ref, w_sem.at[k]).wait()

    def each(fn, *args):
        return lambda: fn(*args)

    pre = {0: [each(own_in, 0), ids_own, each(weights_in, wgu.at[pl.ds(0, first_exp)], 0)],
           1: [each(own_in, 1), each(far_in, 1)],
           2: [ids_far, each(own_in, 2), each(far_in, 3), each(far_ready, 0)],
           3: [each(own_in, 3), each(far_in, 5), each(far_pair_in, 3), each(pair_part, 2), each(far_sum, 0), each(far_ready, 1), each(pair_part, 0), each(pair_part, 1)],
           4: [each(far_pair_in, 5), each(line, (0, ), (), ()), each(far_ready, 2, 3)],
           5: [each(whole_in, 7), each(line, (4, ), (), ()), each(far_ready, 4, 5)],
           6: [each(own_in, 6), each(whole_pair_in, 6), each(line, (7, ), (3, ), ())],
           7: [each(line, (11, ), (7, ), (3, )), each(far_ready, 6, 7)]}
    early = {0: [each(weights_in, wgu.at[pl.ds(first_exp, local_exp - first_exp)], 1)],
           2: [each(far_in, 4)],
           3: [each(far_in, 6), each(far_pair_in, 4)],
           4: [each(whole_in, 6), each(pair_part, 3), each(far_sum, 1), each(line, (1, 2, ), (), ())],
           5: [each(pair_part, 4), each(far_sum, 2), each(far_sum, 3), each(line, (5, ), (0, 1, ), ())],
           6: [each(line, (8, 9, ), (4, ), (0, ))],
           7: [each(pair_part, 6), each(line, (12, 13, ), (8, ), (4, ))]}
    mid = {0: [each(weights_in, wd, 2), each(far_in, 0)],
           1: [each(far_in, 2), each(far_pair_in, 0), each(far_pair_in, 1)],
           2: [each(far_pair_in, 2)],
           4: [each(far_pair_in, 6), each(line, (3, ), (), ())],
           5: [each(line, (6, ), (2, ), ())],
           6: [each(whole_pair_in, 7), each(pair_part, 5), each(far_sum, 4), each(far_sum, 5), each(line, (10, ), (5, 6, ), (1, 2, ))],
           7: [each(line, (14, ), (9, 10, ), (5, 6, ))]}
    out_from, join_from, lag = 15, 11, 4
    sums_out, sums_in = 18, 18

    def run(tasks, step):
        for k, fns in tasks.items():
            @pl.when(step == k)
            def _(fns=fns):
                for fn in fns:
                    fn()

    def chosen_of(tile):
        expert = lax.broadcasted_iota(jnp.int32, (n_experts, mine), 0)
        hit = jnp.zeros((n_experts, mine), jnp.float32)
        for j in range(tile.shape[0]):
            hit = jnp.where(tile[j:j + 1, :] == expert, 1.0, hit)
        return jnp.concatenate([hit, jnp.zeros((128 - n_experts, mine), jnp.float32)], axis=0).T

    @pl.loop(0, n_job)
    def _(step):
        run(pre, step)
        x = v.at[step]
        logits = jnp.dot(x[...], wr[...], preferred_element_type=jnp.float32)
        lane = lax.broadcasted_iota(jnp.int32, logits.shape, 1)
        logits = jnp.where(lane < n_experts, logits, -jnp.inf)
        raised = jnp.exp(logits - jnp.max(logits, axis=-1, keepdims=True))
        prob = raised / jnp.sum(raised, axis=-1, keepdims=True)
        chosen = jnp.concatenate([chosen_of(ids_slot[step, 0]), chosen_of(ids_slot[step, 1])], axis=0)
        gates = pltpu.roll(prob * chosen, (128 - ep * local_exp) % 128, axis=1)
        for e in range(local_exp):
            gu = jnp.dot(x[...], wgu[e], preferred_element_type=jnp.float32)
            if e == local_exp // 2:
                run(early, step)
            a = (jax.nn.silu(gu[:, :width]) * gu[:, width:]).astype(jnp.bfloat16).astype(jnp.float32)
            act[:, e * width:(e + 1) * width] = (a * gates[:, e:e + 1]).astype(jnp.bfloat16)
        run(mid, step)
        for n in range(dim // COLS):
            part = jnp.dot(act[...], wd[:, n * COLS:(n + 1) * COLS], preferred_element_type=jnp.float32)
            keep[step, :, n * COLS:(n + 1) * COLS] = part[:mine]
            dsend[step, :, n * COLS:(n + 1) * COLS] = part[mine:].astype(jnp.bfloat16)
        for n in range(dim // COLS):
            pd(step, n).start()

    def last_sums():
        pair_part(7)
        far_sum(6)
        far_sum(7)

    def pieces_from(first, sums_at, fn):
        for b in range(first // per_blk, N_BLK):
            stops = sorted({max(first - b * per_blk, 0), per_blk} | ({sums_at - b * per_blk} if sums_at // per_blk == b else set()))
            for lo, hi in zip(stops, stops[1:]):
                if b * per_blk + lo == sums_at:
                    last_sums()

                @pl.loop(lo, hi)
                def _(i, b=b):
                    fn(b, i)

    @pl.when(outer)
    def _():
        pieces_from(out_from, sums_out, send_out)

        @pl.loop(0, n_piece)
        def _(p):
            rc(p).wait_recv()

    @pl.when(inner)
    def _():
        def step_in(b, i):
            join_in(b, i)
            finish(b * per_blk + i - lag)

        pieces_from(join_from, sums_in, step_in)
        for p in range(n_piece - lag, n_piece):
            finish(p)

    remote(ids_all, ids_all, ids_s, ids_r.at[0], ep=ep_pair).wait_send()
    two, shared, whole = v.at[pl.ds(0, 2)], v.at[0, pl.ds(0, WHOLE * half)], v.at[0, pl.ds(0, (N_BLK - WHOLE) * blk)]
    remote(two, two, d1_s, d1_r.at[0], ep=ep_pair).wait_send()
    remote(shared, shared, dy_s, dy_r.at[0], ep=ep_far).wait_send()
    remote(shared, shared, dz_s, dz_r.at[0], tp=z_pair).wait_send()
    remote(two, two, dd_s, dd_r.at[0], ep=ep_pair).wait_send()
    remote(dsend, drecv, pd_s, pd_r.at[0], ep=ep_pair).wait_send()
    remote(sbuf, rbuf, sy_s, sy_r.at[0], ep=ep_far).wait_send()

    @pl.when(outer)
    def _():
        remote(tbuf, abuf, rac_s, rac_r.at[0], tp=z_pair).wait_send()

    @pl.when(inner)
    def _():
        remote(whole, whole, dyw_s, dyw_r.at[0], ep=ep_far).wait_send()
        remote(whole, whole, dzw_s, dzw_r.at[0], tp=z_pair).wait_send()
        remote(tbuf, ubuf, rb_s, rb_r.at[0], tp=z_mirror).wait_send()
        remote(out_ref, out_ref, rac_s, rac_r.at[0], tp=z_pair).wait_send()


def solution(mesh):
    def per_device(hidden, expert_ids, norm_w, router_w, w_gate, w_up, w_down):
        tok, dim = hidden.shape
        top_k = expert_ids.shape[1]
        local_exp, _, width = w_gate.shape
        blk = tok // N_BLK
        n_job = len(JOBS)
        n_piece = tok // PIECE
        ids_t = expert_ids.reshape(N_BLK // 2, 2 * blk, top_k).transpose(0, 2, 1)
        bf, f32 = jnp.bfloat16, jnp.float32
        dma = pltpu.SemaphoreType.DMA
        scratch = [
            pltpu.VMEM((N_BLK // 2, top_k, 2 * blk), jnp.int32),
            pltpu.VMEM((dim,), bf),
            pltpu.VMEM((router_w.shape[1], dim), bf),
            pltpu.VMEM((tok, dim), bf),
            pltpu.VMEM((dim, 128), bf),
            pltpu.VMEM((n_job, 4 * blk, dim), bf),
            pltpu.VMEM((local_exp, dim, 2 * width), bf),
            pltpu.VMEM((local_exp * width, dim), bf),
            pltpu.VMEM((4 * blk, local_exp * width), bf),
            pltpu.VMEM((n_job, 2 * blk, dim), f32),
            pltpu.VMEM((n_job, 2 * blk, dim), bf),
            pltpu.VMEM((n_job, 2 * blk, dim), bf),
            pltpu.VMEM((tok, dim), bf),
            pltpu.VMEM((tok, dim), bf),
            pltpu.VMEM((tok, dim), bf),
            pltpu.VMEM((tok, dim), bf),
            pltpu.VMEM((tok, dim), bf),
            pltpu.VMEM((3, N_BLK // 2, top_k, 2 * blk), jnp.int32),
            pltpu.VMEM((n_job, 2, top_k, 2 * blk), jnp.int32),
            dma((tok // (2 * blk) + 3,)),
            dma((3,)),
            dma, dma((3,)),
            dma, dma((n_job,)),
            dma, dma((len(UNITS),)),
            dma, dma((len(UNITS),)),
            dma, dma((N_BLK - WHOLE,)),
            dma, dma((N_BLK - WHOLE,)),
            dma, dma((N_BLK,)),
            dma, dma((n_job,)),
            dma, dma((n_piece,)),
            dma, dma((n_piece,)),
            dma, dma((n_piece,)),
        ]
        operands = (ids_t, hidden, norm_w, router_w.T, w_gate, w_up, w_down.reshape(local_exp * width, dim))
        return pl.pallas_call(
            body,
            out_shape=jax.ShapeDtypeStruct((tok, dim), bf),
            in_specs=[pl.BlockSpec(memory_space=pltpu.HBM)] * len(operands),
            out_specs=pl.BlockSpec(memory_space=pltpu.VMEM),
            scratch_shapes=scratch,
            compiler_params=pltpu.CompilerParams(collective_id=0, has_side_effects=True, vmem_limit_bytes=53_000_000),
            name="moe_layer",
        )(*[pltpu.with_memory_space_constraint(x, pltpu.HBM) for x in operands])

    token_spec = P(("dp", "ep"), None)
    return jax.shard_map(per_device, mesh=mesh, in_specs=(token_spec, token_spec, P(None), P(None, None), P("ep", None, "tp"), P("ep", None, "tp"), P("ep", "tp", None)), out_specs=token_spec, check_vma=False)
```

```python
import jax
import jax.numpy as jnp
from jax import lax
from jax.experimental import pallas as pl
from jax.experimental.pallas import tpu as pltpu
from jax.sharding import PartitionSpec as P

NORM_EPS = 1e-6
MESH = pl.DeviceIdType.MESH
N_BLK = 8
PIECE = 16
COLS = 512
JOBS = (
    (("own", 0), ("own", 1)),
    (("own", 2), ("own", 3)),
    (("far", 0), ("own", 4)),
    (("far", 1), ("own", 5)),
    (("far", 2), ("far", 3)),
    (("far", 4), ("far", 5)),
    (("own", 6), ("own", 7)),
    (("far", 6), ("far", 7)),
)
OWN_JOBS = tuple(slot for slot, job in enumerate(JOBS) if any(kind == "own" for kind, _ in job))
PLACE = {block: (slot, k) for slot, job in enumerate(JOBS) for k, block in enumerate(job)}
WHOLE = 6
UNITS = ((0, 0, 16), (0, 16, 16)) + tuple((b, 0, 32) for b in range(1, WHOLE))


def body(ids_hbm, h_hbm, nw_hbm, wrt_hbm, wg_hbm, wu_hbm, wd_hbm, out_ref,
         ids_ref, nw_ref, wrt_ref, h_ref, wr, v, wgu, wd, act, keep, dsend, drecv, sbuf, rbuf, tbuf, abuf, ubuf, ids_all, ids_slot,
         h_sem, w_sem, ids_s, ids_r, d1_s, d1_r, dy_s, dy_r, dz_s, dz_r, dyw_s, dyw_r, dzw_s, dzw_r, dd_s, dd_r, pd_s, pd_r,
         sy_s, sy_r, rac_s, rac_r, rb_s, rb_r):
    tok, dim = h_ref.shape
    n_experts = wrt_ref.shape[0]
    local_exp, _, width = wg_hbm.shape
    blk = tok // N_BLK
    half = blk // 2
    mine = 2 * blk
    n_job = len(JOBS)
    n_piece = tok // PIECE
    per_blk = blk // PIECE
    ep = lax.axis_index("ep")
    z = lax.axis_index("tp")
    core, y = ep % 2, ep // 2
    ep_pair = 2 * y + 1 - core
    ep_far = 2 * (1 - y) + core
    ep_diag = 2 * (1 - y) + 1 - core
    side = z % 2
    z_pair = z + 1 - 2 * side
    z_mirror = 3 - z
    inner = jnp.logical_or(z == 1, z == 2)
    outer = jnp.logical_or(z == 0, z == 3)

    def remote(src, dst, ssem, rsem, **where):
        return pltpu.make_async_remote_copy(src_ref=src, dst_ref=dst, send_sem=ssem, recv_sem=rsem, device_id=where, device_id_type=MESH)

    first_exp = local_exp // 2 + 1

    def weight_copies():
        copies = []
        for e in range(local_exp):
            copies.append(pltpu.make_async_copy(wg_hbm.at[e], wgu.at[e, :, pl.ds(0, width)], w_sem.at[e // first_exp]))
            copies.append(pltpu.make_async_copy(wu_hbm.at[e], wgu.at[e, :, pl.ds(width, width)], w_sem.at[e // first_exp]))
        copies.append(pltpu.make_async_copy(wd_hbm, wd, w_sem.at[2]))
        return copies

    def h_copy(k):
        rows = pl.ds(k * mine, mine)
        return pltpu.make_async_copy(h_hbm.at[rows], h_ref.at[rows], h_sem.at[k])

    n_h = tok // mine
    small = [pltpu.make_async_copy(src, dst, h_sem.at[n_h + k]) for k, (src, dst) in enumerate(((nw_hbm, nw_ref), (ids_hbm, ids_ref), (wrt_hbm, wrt_ref)))]
    h_copy(0).start()
    for copy in small:
        copy.start()
    for k in range(1, n_h):
        h_copy(k).start()
    barrier = pltpu.get_barrier_semaphore()
    for where in ({"ep": ep_pair}, {"ep": ep_far}, {"ep": ep_diag}, {"tp": z_pair}):
        pl.semaphore_signal(barrier, inc=1, device_id=where, device_id_type=MESH)

    @pl.when(inner)
    def _():
        pl.semaphore_signal(barrier, inc=1, device_id={"tp": z_mirror}, device_id_type=MESH)

    for copy in weight_copies():
        copy.start()

    small[0].wait()
    scale = nw_ref[...].astype(jnp.float32).reshape(1, dim)

    def norm_block(b):
        slot, k = PLACE["own", b]
        if b % 2 == 0:
            h_copy(b // 2).wait()

        def group(i, carry):
            r = pl.multiple_of(i * 16, 16)
            x = h_ref[pl.ds(b * blk + r, 16), :].astype(jnp.float32)
            ms = jnp.mean(x * x, axis=-1, keepdims=True)
            v[slot, pl.ds(k * blk + r, 16), :] = (x * lax.rsqrt(ms + NORM_EPS) * scale).astype(jnp.bfloat16)
            return carry

        lax.fori_loop(0, blk // 16, group, 0, unroll=True)

    def unit(kind, u, which, base=0):
        b, first, rows = UNITS[u]
        slot, k = PLACE[kind, b]
        return v.at[slot, pl.ds(pl.multiple_of(base + k * blk + which * half + first, 16), rows)]

    def block(kind, b, base=0):
        slot, k = PLACE[kind, b]
        return v.at[slot, pl.ds(base + k * blk, blk)]

    def ids_copy(k):
        ep_to = (ep_pair, ep_far, ep_diag)[k]
        return remote(ids_ref, ids_all.at[k], ids_s, ids_r.at[k], ep=ep_to)

    def d1(b):
        return remote(block("own", b), block("own", b, mine), d1_s, d1_r.at[OWN_JOBS.index(PLACE["own", b][0])], ep=ep_pair)

    def dy(u):
        return remote(unit("own", u, side), unit("far", u, side), dy_s, dy_r.at[u], ep=ep_far)

    def dz(u, which):
        return remote(unit("far", u, which), unit("far", u, which), dz_s, dz_r.at[u], tp=z_pair)

    def dd(u, which):
        return remote(unit("far", u, which), unit("far", u, which, mine), dd_s, dd_r.at[UNITS[u][0]], ep=ep_pair)

    def dy_whole(b):
        return remote(block("own", b), block("far", b), dyw_s, dyw_r.at[b - WHOLE], ep=ep_far)

    def dz_whole(b):
        return remote(block("far", b), block("far", b), dzw_s, dzw_r.at[b - WHOLE], tp=z_pair)

    def dd_whole(b):
        return remote(block("far", b), block("far", b, mine), dd_s, dd_r.at[b], ep=ep_pair)

    def pd(slot, n):
        cols = pl.ds(n * COLS, COLS)
        return remote(dsend.at[slot, :, cols], drecv.at[slot, :, cols], pd_s, pd_r.at[slot], ep=ep_pair)

    def piece_rows(p):
        return pl.ds(pl.multiple_of(p * PIECE, PIECE), PIECE)

    def sy(p):
        return remote(sbuf.at[piece_rows(p)], rbuf.at[piece_rows(p)], sy_s, sy_r.at[p], ep=ep_far)

    def ra(p):
        return remote(tbuf.at[piece_rows(p)], abuf.at[piece_rows(p)], rac_s, rac_r.at[p], tp=z_pair)

    def rb(p):
        return remote(tbuf.at[piece_rows(p)], ubuf.at[piece_rows(p)], rb_s, rb_r.at[p], tp=z_mirror)

    def rc(p):
        return remote(out_ref.at[piece_rows(p)], out_ref.at[piece_rows(p)], rac_s, rac_r.at[p], tp=z_pair)

    for b in range(N_BLK):
        norm_block(b)
        if b == 0:
            pl.semaphore_wait(barrier, jnp.where(inner, 5, 4))
        for u, (of, _, _) in enumerate(UNITS):
            if of == b:
                dy(u).start()
        if b >= WHOLE:
            @pl.when(inner)
            def _(b=b):
                dy_whole(b).start()
        d1(b).start()
        if b == 0:
            small[1].wait()
            for k in range(3):
                ids_copy(k).start()

    def own_in(slot):
        of_job = [b for kind, b in JOBS[slot] if kind == "own"]
        rows = v.at[slot, pl.ds(mine + PLACE["own", of_job[0]][1] * blk, len(of_job) * blk)]
        remote(rows, rows, d1_s, d1_r.at[OWN_JOBS.index(slot)], ep=ep_pair).wait_recv()

    def far_in(u):
        dy(u).wait_recv()
        dz(u, side).start()
        dd(u, side).start()

    def far_pair_in(u):
        dz(u, 1 - side).wait_recv()
        dd(u, 1 - side).start()

    def whole_in(b):
        @pl.when(inner)
        def _():
            dy_whole(b).wait_recv()
            dz_whole(b).start()
            dd_whole(b).start()

    def whole_pair_in(b):
        @pl.when(outer)
        def _():
            dz_whole(b).wait_recv()
            dd_whole(b).start()

    def far_ready(*blocks):
        for b in blocks:
            remote(block("far", b), block("far", b, mine), dd_s, dd_r.at[b], ep=ep_pair).wait_recv()

    def ids_own():
        ids_copy(0).wait_recv()
        for b in range(N_BLK):
            slot, k = PLACE["own", b]
            lanes, at = slice(b % 2 * blk, (b % 2 + 1) * blk), slice(k * blk, (k + 1) * blk)
            ids_slot[slot, 0, :, at] = ids_ref[b // 2, :, lanes]
            ids_slot[slot, 1, :, at] = ids_all[0, b // 2, :, lanes]

    def ids_far():
        ids_copy(1).wait_recv()
        ids_copy(2).wait_recv()
        for b in range(N_BLK):
            slot, k = PLACE["far", b]
            lanes, at = slice(b % 2 * blk, (b % 2 + 1) * blk), slice(k * blk, (k + 1) * blk)
            ids_slot[slot, 0, :, at] = ids_all[1, b // 2, :, lanes]
            ids_slot[slot, 1, :, at] = ids_all[2, b // 2, :, lanes]

    def pair_part(slot):
        remote(dsend.at[slot], drecv.at[slot], pd_s, pd_r.at[slot], ep=ep_pair).wait_recv()

    def far_sum(b):
        slot, k = PLACE["far", b]

        def one(i, carry):
            rows = pl.ds(pl.multiple_of(k * blk + i * PIECE, PIECE), PIECE)
            total = keep[slot, rows, :] + drecv[slot, rows, :].astype(jnp.float32)
            sbuf[piece_rows(b * per_blk + i), :] = total.astype(jnp.bfloat16)
            sy(b * per_blk + i).start()
            return carry

        lax.fori_loop(0, per_blk, one, 0)

    small[2].wait()
    wide = jnp.concatenate([wrt_ref[...].astype(jnp.float32), jnp.zeros((128 - n_experts, dim), jnp.float32)], axis=0)
    wr[...] = wide.T.astype(jnp.bfloat16)

    def total_of(b, i):
        slot, k = PLACE["own", b]
        p = b * per_blk + i
        sy(p).wait_recv()
        rows = pl.ds(pl.multiple_of(k * blk + i * PIECE, PIECE), PIECE)
        return keep[slot, rows, :] + drecv[slot, rows, :].astype(jnp.float32) + rbuf[piece_rows(p), :].astype(jnp.float32)

    def send_out(b, i):
        p = b * per_blk + i
        tbuf[piece_rows(p), :] = total_of(b, i).astype(jnp.bfloat16)
        ra(p).start()

    def join_in(b, i):
        p = b * per_blk + i
        total = total_of(b, i)
        ra(p).wait_recv()
        tbuf[piece_rows(p), :] = (total + abuf[piece_rows(p), :].astype(jnp.float32)).astype(jnp.bfloat16)
        rb(p).start()

    def finish(p):
        rb(p).wait_recv()
        rows = piece_rows(p)
        total = tbuf[rows, :].astype(jnp.float32) + ubuf[rows, :].astype(jnp.float32)
        out_ref[rows, :] = (h_ref[rows, :].astype(jnp.float32) + total).astype(jnp.bfloat16)
        rc(p).start()

    def line(out=(), joined=(), done=()):
        @pl.when(outer)
        def _():
            for p in out:
                send_out(*divmod(p, per_blk))

        @pl.when(inner)
        def _():
            for p in joined:
                join_in(*divmod(p, per_blk))
            for p in done:
                finish(p)

    def weights_in(ref, k):
        pltpu.make_async_copy(ref, ref, w_sem.at[k]).wait()

    def each(fn, *args):
        return lambda: fn(*args)

    pre = {0: [each(own_in, 0), ids_own, each(weights_in, wgu.at[pl.ds(0, first_exp)], 0)],
           1: [each(own_in, 1), each(far_in, 1)],
           2: [ids_far, each(own_in, 2), each(far_in, 3), each(far_ready, 0)],
           3: [each(own_in, 3), each(far_in, 5), each(far_pair_in, 3), each(pair_part, 2), each(far_sum, 0), each(far_ready, 1), each(pair_part, 0), each(pair_part, 1)],
           4: [each(far_pair_in, 5), each(line, (0, ), (), ()), each(far_ready, 2, 3)],
           5: [each(whole_in, 7), each(line, (4, ), (), ()), each(far_ready, 4, 5)],
           6: [each(own_in, 6), each(whole_pair_in, 6), each(line, (7, ), (3, ), ())],
           7: [each(line, (11, ), (7, ), (3, )), each(far_ready, 6, 7)]}
    early = {0: [each(weights_in, wgu.at[pl.ds(first_exp, local_exp - first_exp)], 1)],
           2: [each(far_in, 4)],
           3: [each(far_in, 6), each(far_pair_in, 4)],
           4: [each(whole_in, 6), each(pair_part, 3), each(far_sum, 1), each(line, (1, 2, ), (), ())],
           5: [each(pair_part, 4), each(far_sum, 2), each(far_sum, 3), each(line, (5, ), (0, 1, ), ())],
           6: [each(line, (8, 9, ), (4, ), (0, ))],
           7: [each(pair_part, 6), each(line, (12, 13, ), (8, ), (4, ))]}
    mid = {0: [each(weights_in, wd, 2), each(far_in, 0)],
           1: [each(far_in, 2), each(far_pair_in, 0), each(far_pair_in, 1)],
           2: [each(far_pair_in, 2)],
           4: [each(far_pair_in, 6), each(line, (3, ), (), ())],
           5: [each(line, (6, ), (2, ), ())],
           6: [each(whole_pair_in, 7), each(pair_part, 5), each(far_sum, 4), each(far_sum, 5), each(line, (10, ), (5, 6, ), (1, 2, ))],
           7: [each(line, (14, ), (9, 10, ), (5, 6, ))]}
    out_from, join_from, lag = 15, 11, 4
    sums_out, sums_in = 18, 18

    def run(tasks, step):
        for k, fns in tasks.items():
            @pl.when(step == k)
            def _(fns=fns):
                for fn in fns:
                    fn()

    def chosen_of(tile):
        expert = lax.broadcasted_iota(jnp.int32, (n_experts, mine), 0)
        hit = jnp.zeros((n_experts, mine), jnp.float32)
        for j in range(tile.shape[0]):
            hit = jnp.where(tile[j:j + 1, :] == expert, 1.0, hit)
        return jnp.concatenate([hit, jnp.zeros((128 - n_experts, mine), jnp.float32)], axis=0).T

    @pl.loop(0, n_job)
    def _(step):
        run(pre, step)
        x = v.at[step]
        logits = jnp.dot(x[...], wr[...], preferred_element_type=jnp.float32)
        lane = lax.broadcasted_iota(jnp.int32, logits.shape, 1)
        logits = jnp.where(lane < n_experts, logits, -jnp.inf)
        raised = jnp.exp(logits - jnp.max(logits, axis=-1, keepdims=True))
        prob = raised / jnp.sum(raised, axis=-1, keepdims=True)
        chosen = jnp.concatenate([chosen_of(ids_slot[step, 0]), chosen_of(ids_slot[step, 1])], axis=0)
        gates = pltpu.roll(prob * chosen, (128 - ep * local_exp) % 128, axis=1)
        for e in range(local_exp):
            gu = jnp.dot(x[...], wgu[e], preferred_element_type=jnp.float32)
            if e == local_exp // 2:
                run(early, step)
            a = (jax.nn.silu(gu[:, :width]) * gu[:, width:]).astype(jnp.bfloat16).astype(jnp.float32)
            act[:, e * width:(e + 1) * width] = (a * gates[:, e:e + 1]).astype(jnp.bfloat16)
        run(mid, step)
        for n in range(dim // COLS):
            part = jnp.dot(act[...], wd[:, n * COLS:(n + 1) * COLS], preferred_element_type=jnp.float32)
            keep[step, :, n * COLS:(n + 1) * COLS] = part[:mine]
            dsend[step, :, n * COLS:(n + 1) * COLS] = part[mine:].astype(jnp.bfloat16)
        for n in range(dim // COLS):
            pd(step, n).start()

    def last_sums():
        pair_part(7)
        far_sum(6)
        far_sum(7)

    def pieces_from(first, sums_at, fn):
        for b in range(first // per_blk, N_BLK):
            stops = sorted({max(first - b * per_blk, 0), per_blk} | ({sums_at - b * per_blk} if sums_at // per_blk == b else set()))
            for lo, hi in zip(stops, stops[1:]):
                if b * per_blk + lo == sums_at:
                    last_sums()

                @pl.loop(lo, hi)
                def _(i, b=b):
                    fn(b, i)

    @pl.when(outer)
    def _():
        pieces_from(out_from, sums_out, send_out)

        @pl.loop(0, n_piece)
        def _(p):
            rc(p).wait_recv()

    @pl.when(inner)
    def _():
        def step_in(b, i):
            join_in(b, i)
            finish(b * per_blk + i - lag)

        pieces_from(join_from, sums_in, step_in)
        for p in range(n_piece - lag, n_piece):
            finish(p)

    remote(ids_all, ids_all, ids_s, ids_r.at[0], ep=ep_pair).wait_send()
    two, shared, whole = v.at[pl.ds(0, 2)], v.at[0, pl.ds(0, WHOLE * half)], v.at[0, pl.ds(0, (N_BLK - WHOLE) * blk)]
    remote(two, two, d1_s, d1_r.at[0], ep=ep_pair).wait_send()
    remote(shared, shared, dy_s, dy_r.at[0], ep=ep_far).wait_send()
    remote(shared, shared, dz_s, dz_r.at[0], tp=z_pair).wait_send()
    remote(two, two, dd_s, dd_r.at[0], ep=ep_pair).wait_send()
    remote(dsend, drecv, pd_s, pd_r.at[0], ep=ep_pair).wait_send()
    remote(sbuf, rbuf, sy_s, sy_r.at[0], ep=ep_far).wait_send()

    @pl.when(outer)
    def _():
        remote(tbuf, abuf, rac_s, rac_r.at[0], tp=z_pair).wait_send()

    @pl.when(inner)
    def _():
        remote(whole, whole, dyw_s, dyw_r.at[0], ep=ep_far).wait_send()
        remote(whole, whole, dzw_s, dzw_r.at[0], tp=z_pair).wait_send()
        remote(tbuf, ubuf, rb_s, rb_r.at[0], tp=z_mirror).wait_send()
        remote(out_ref, out_ref, rac_s, rac_r.at[0], tp=z_pair).wait_send()


def solution(mesh):
    def per_device(hidden, expert_ids, norm_w, router_w, w_gate, w_up, w_down):
        tok, dim = hidden.shape
        top_k = expert_ids.shape[1]
        local_exp, _, width = w_gate.shape
        blk = tok // N_BLK
        n_job = len(JOBS)
        n_piece = tok // PIECE
        ids_t = expert_ids.reshape(N_BLK // 2, 2 * blk, top_k).transpose(0, 2, 1)
        bf, f32 = jnp.bfloat16, jnp.float32
        dma = pltpu.SemaphoreType.DMA
        scratch = [
            pltpu.VMEM((N_BLK // 2, top_k, 2 * blk), jnp.int32),
            pltpu.VMEM((dim,), bf),
            pltpu.VMEM((router_w.shape[1], dim), bf),
            pltpu.VMEM((tok, dim), bf),
            pltpu.VMEM((dim, 128), bf),
            pltpu.VMEM((n_job, 4 * blk, dim), bf),
            pltpu.VMEM((local_exp, dim, 2 * width), bf),
            pltpu.VMEM((local_exp * width, dim), bf),
            pltpu.VMEM((4 * blk, local_exp * width), bf),
            pltpu.VMEM((n_job, 2 * blk, dim), f32),
            pltpu.VMEM((n_job, 2 * blk, dim), bf),
            pltpu.VMEM((n_job, 2 * blk, dim), bf),
            pltpu.VMEM((tok, dim), bf),
            pltpu.VMEM((tok, dim), bf),
            pltpu.VMEM((tok, dim), bf),
            pltpu.VMEM((tok, dim), bf),
            pltpu.VMEM((tok, dim), bf),
            pltpu.VMEM((3, N_BLK // 2, top_k, 2 * blk), jnp.int32),
            pltpu.VMEM((n_job, 2, top_k, 2 * blk), jnp.int32),
            dma((tok // (2 * blk) + 3,)),
            dma((3,)),
            dma, dma((3,)),
            dma, dma((len(OWN_JOBS),)),
            dma, dma((len(UNITS),)),
            dma, dma((len(UNITS),)),
            dma, dma((N_BLK - WHOLE,)),
            dma, dma((N_BLK - WHOLE,)),
            dma, dma((N_BLK,)),
            dma, dma((n_job,)),
            dma, dma((n_piece,)),
            dma, dma((n_piece,)),
            dma, dma((n_piece,)),
        ]
        operands = (ids_t, hidden, norm_w, router_w.T, w_gate, w_up, w_down.reshape(local_exp * width, dim))
        return pl.pallas_call(
            body,
            out_shape=jax.ShapeDtypeStruct((tok, dim), bf),
            in_specs=[pl.BlockSpec(memory_space=pltpu.HBM)] * len(operands),
            out_specs=pl.BlockSpec(memory_space=pltpu.VMEM),
            scratch_shapes=scratch,
            compiler_params=pltpu.CompilerParams(collective_id=0, has_side_effects=True, vmem_limit_bytes=53_000_000),
            name="moe_layer",
        )(*[pltpu.with_memory_space_constraint(x, pltpu.HBM) for x in operands])

    token_spec = P(("dp", "ep"), None)
    return jax.shard_map(per_device, mesh=mesh, in_specs=(token_spec, token_spec, P(None), P(None, None), P("ep", None, "tp"), P("ep", None, "tp"), P("ep", "tp", None)), out_specs=token_spec, check_vma=False)
```
